32 devices in a mesh: dp: 4 (over y, z), tp: 8 (over x, core).
Axes of the slice: x: 4, y: 2, z: 2, core: 2. Of those that a mesh axis runs over, the one named last changes fastest.
The devices are a block of a 4x4x8 slice.
Arguments:
- tokens: int32 [4, 512], P('dp'), parts along dimension 0
- positions: int32 [4, 512], P('dp'), parts along dimension 0
- embed_table: bfloat16 [128256, 3072], P('tp')
- w_query: bfloat16 [3072, 24, 128], P(None, 'tp')
- w_key: bfloat16 [3072, 8, 128], P(None, 'tp')
- w_value: bfloat16 [3072, 8, 128], P(None, 'tp')
- w_out: bfloat16 [24, 128, 3072], P('tp')
- w_gate: bfloat16 [3072, 8192], P(None, 'tp')
- w_up: bfloat16 [3072, 8192], P(None, 'tp')
- w_down: bfloat16 [8192, 3072], P('tp')
- norm_pre_att: float32 [3072], replicated
- norm_post_att: float32 [3072], replicated
- norm_pre_ffw: float32 [3072], replicated
- norm_post_ffw: float32 [3072], replicated
Outputs:
- output: bfloat16 [4, 512, 3072], P('dp', 'tp'), parts along dimension 0
There are 4 independent parts. The reference program is written for one: setup_inputs(seed, part) draws one part's arguments, and reference() takes and returns one part's arrays. A program takes and returns all parts, laid end to end along the dimension named above; an argument that names none is the same for every part.
All inputs are finite; a program needn't handle non-finite values.
Results may differ from the reference program's by a relative error of at most 0.02.
Values are sent between devices in bfloat16 or wider.
A program may use at most 768 MiB of HBM per device.

```python
import jax
import jax.numpy as jnp
from jax import lax

BATCH_SIZE = 1
SEQ_LEN = 512
MODEL_DIM = 3072
N_HEADS = 24
KV_HEADS = 8
HEAD_DIM = 128
FFN_DIM = 8192
VOCAB_SIZE = 128256
WINDOW = 4096
QUERY_SCALAR = 256

GROUP_SIZE = N_HEADS // KV_HEADS
QUERY_BLOCK = min(128, SEQ_LEN)
KEY_SPAN = min(SEQ_LEN, WINDOW + QUERY_BLOCK)
SOFT_CAP = 50.0
NORM_EPS = 1e-6
ROPE_BASE = 10000.0


def setup_inputs(seed: int = 0, part: int = 0) -> dict:
    root_key = jax.random.key(seed)
    key_list = jax.random.split(root_key, 11)
    part_keys = jax.random.split(jax.random.fold_in(root_key, part), 5)
    grid_shape = (BATCH_SIZE, SEQ_LEN)
    choice = jax.random.randint(part_keys[0], grid_shape, 0, 4, dtype=jnp.int32)
    hot_ids = jax.random.randint(part_keys[1], grid_shape, 0, VOCAB_SIZE // 4, dtype=jnp.int32)
    any_ids = jax.random.randint(part_keys[2], grid_shape, 0, VOCAB_SIZE, dtype=jnp.int32)
    tokens = jnp.where(choice < 3, hot_ids, any_ids)
    tokens = tokens.at[0, 0].set(VOCAB_SIZE - 1).at[0, 1].set(0)
    pos_step = max(1, (2 * WINDOW) // SEQ_LEN)
    pos_gaps = jax.random.randint(part_keys[3], grid_shape, 1, 2 * pos_step + 1, dtype=jnp.int32)
    first_pos = jax.random.randint(part_keys[4], (BATCH_SIZE, 1), 0, WINDOW, dtype=jnp.int32)
    positions = (first_pos + jnp.cumsum(pos_gaps, axis=1) - pos_gaps[:, :1]).astype(jnp.int32)

    def draw_weight(key_index, w_shape, fan_in):
        raw_noise = jax.random.normal(key_list[key_index], w_shape, jnp.float32)
        return (raw_noise * fan_in ** -0.5).astype(jnp.bfloat16)

    def table_rows(row_group):
        raw_noise = jax.random.normal(jax.random.fold_in(key_list[0], row_group), (VOCAB_SIZE // 8, MODEL_DIM), jnp.float32)
        return (raw_noise * MODEL_DIM ** -0.5).astype(jnp.bfloat16)

    embed_table = lax.map(table_rows, jnp.arange(8)).reshape(VOCAB_SIZE, MODEL_DIM)
    norm_draws = 0.3 * jax.random.normal(key_list[8], (4, MODEL_DIM), jnp.float32)
    return {
        "tokens": tokens,
        "positions": positions,
        "embed_table": embed_table,
        "w_query": draw_weight(1, (MODEL_DIM, N_HEADS, HEAD_DIM), MODEL_DIM),
        "w_key": draw_weight(2, (MODEL_DIM, KV_HEADS, HEAD_DIM), MODEL_DIM),
        "w_value": draw_weight(3, (MODEL_DIM, KV_HEADS, HEAD_DIM), MODEL_DIM),
        "w_out": draw_weight(4, (N_HEADS, HEAD_DIM, MODEL_DIM), N_HEADS * HEAD_DIM),
        "w_gate": draw_weight(5, (MODEL_DIM, FFN_DIM), MODEL_DIM),
        "w_up": draw_weight(6, (MODEL_DIM, FFN_DIM), MODEL_DIM),
        "w_down": draw_weight(7, (FFN_DIM, MODEL_DIM), FFN_DIM),
        "norm_pre_att": norm_draws[0],
        "norm_post_att": norm_draws[1],
        "norm_pre_ffw": norm_draws[2],
        "norm_post_ffw": norm_draws[3],
    }


def rms_norm(hidden, norm_scale):
    hidden = hidden.astype(jnp.float32)
    mean_sq = jnp.mean(hidden * hidden, axis=-1, keepdims=True)
    return (hidden * lax.rsqrt(mean_sq + NORM_EPS) * (1.0 + norm_scale)).astype(jnp.bfloat16)


def apply_rope(states, positions):
    half_dim = HEAD_DIM // 2
    inv_freq = ROPE_BASE ** (-2.0 * jnp.arange(half_dim, dtype=jnp.float32) / HEAD_DIM)
    angles = positions.astype(jnp.float32)[:, :, None] * inv_freq
    cos_tab = jnp.cos(angles)[:, :, None, :]
    sin_tab = jnp.sin(angles)[:, :, None, :]
    lower_half = states[..., :half_dim]
    upper_half = states[..., half_dim:]
    return jnp.concatenate([lower_half * cos_tab - upper_half * sin_tab, upper_half * cos_tab + lower_half * sin_tab], axis=-1)


def project(act_rows, weight, out_shape):
    flat_rows = act_rows.reshape(-1, act_rows.shape[-1])
    flat_w = weight.reshape(act_rows.shape[-1], -1)
    return jnp.dot(flat_rows, flat_w, preferred_element_type=jnp.float32).reshape(out_shape)


def attend(q_states, k_states, v_states, positions):
    n_blocks = SEQ_LEN // QUERY_BLOCK

    def one_block(block_idx):
        q_start = block_idx * QUERY_BLOCK
        k_start = jnp.maximum(q_start + QUERY_BLOCK - KEY_SPAN, 0)
        q_blk = lax.dynamic_slice_in_dim(q_states, q_start, QUERY_BLOCK, axis=1)
        k_blk = lax.dynamic_slice_in_dim(k_states, k_start, KEY_SPAN, axis=1)
        v_blk = lax.dynamic_slice_in_dim(v_states, k_start, KEY_SPAN, axis=1)
        q_pos = lax.dynamic_slice_in_dim(positions, q_start, QUERY_BLOCK, axis=1)
        k_pos = lax.dynamic_slice_in_dim(positions, k_start, KEY_SPAN, axis=1)
        scores = jnp.einsum("bqkgd,blkd->bkgql", q_blk.astype(jnp.float32), k_blk.astype(jnp.float32))
        capped = SOFT_CAP * jnp.tanh(scores / SOFT_CAP)
        offset = q_pos[:, :, None] - k_pos[:, None, :]
        keep_mask = (offset >= 0) & (offset < WINDOW)
        capped = jnp.where(keep_mask[:, None, None, :, :], capped, -1e30)
        att_probs = jax.nn.softmax(capped, axis=-1).astype(jnp.bfloat16)
        att_mix = jnp.einsum("bkgql,blkd->bqkgd", att_probs.astype(jnp.float32), v_blk.astype(jnp.float32))
        return att_mix.astype(jnp.bfloat16)

    blocks = lax.map(one_block, jnp.arange(n_blocks))
    return jnp.moveaxis(blocks, 0, 1).reshape(BATCH_SIZE, SEQ_LEN, KV_HEADS, GROUP_SIZE, HEAD_DIM)


def reference(tokens, positions, embed_table, w_query, w_key, w_value, w_out, w_gate, w_up, w_down, norm_pre_att, norm_post_att, norm_pre_ffw, norm_post_ffw):
    normalizer = jnp.sqrt(jnp.float32(MODEL_DIM)).astype(jnp.bfloat16).astype(jnp.float32)
    looked = jnp.take(embed_table, tokens, axis=0)
    embeds = (looked.astype(jnp.float32) * normalizer).astype(jnp.bfloat16)
    attn_in = rms_norm(embeds, norm_pre_att)
    heads_shape = (BATCH_SIZE, SEQ_LEN, N_HEADS, HEAD_DIM)
    kv_shape = (BATCH_SIZE, SEQ_LEN, KV_HEADS, HEAD_DIM)
    q_states = apply_rope(project(attn_in, w_query, heads_shape), positions) * QUERY_SCALAR ** -0.5
    q_states = q_states.astype(jnp.bfloat16).reshape(BATCH_SIZE, SEQ_LEN, KV_HEADS, GROUP_SIZE, HEAD_DIM)
    k_states = apply_rope(project(attn_in, w_key, kv_shape), positions).astype(jnp.bfloat16)
    v_states = project(attn_in, w_value, kv_shape).astype(jnp.bfloat16)
    att_mix = attend(q_states, k_states, v_states, positions)
    model_shape = (BATCH_SIZE, SEQ_LEN, MODEL_DIM)
    att_flat = att_mix.reshape(BATCH_SIZE, SEQ_LEN, N_HEADS * HEAD_DIM)
    att_proj = project(att_flat, w_out, model_shape).astype(jnp.bfloat16)
    resid_one = (embeds.astype(jnp.float32) + rms_norm(att_proj, norm_post_att).astype(jnp.float32)).astype(jnp.bfloat16)
    mlp_in = rms_norm(resid_one, norm_pre_ffw)
    ffn_shape = (BATCH_SIZE, SEQ_LEN, FFN_DIM)
    gate_pre = project(mlp_in, w_gate, ffn_shape)
    up_proj = project(mlp_in, w_up, ffn_shape)
    ffn_act = (jax.nn.gelu(gate_pre, approximate=True) * up_proj).astype(jnp.bfloat16)
    down_proj = project(ffn_act, w_down, model_shape).astype(jnp.bfloat16)
    return (resid_one.astype(jnp.float32) + rms_norm(down_proj, norm_post_ffw).astype(jnp.float32)).astype(jnp.bfloat16)
```

```python
import functools

import jax
import jax.numpy as jnp
from jax import lax
from jax.experimental import pallas as pl
from jax.experimental.pallas import tpu as pltpu
from jax.sharding import PartitionSpec as P

WINDOW = 4096
QUERY_SCALE = 256.0 ** -0.5
SOFT_CAP = 50.0
NORM_EPS = 1e-6
ROPE_BASE = 10000.0
MESH = pl.DeviceIdType.MESH
BF16 = jnp.bfloat16
F32 = jnp.float32
PIECES = 4
NT = (((1,), (1,)), ((), ()))


def norm_rows(hidden, scale):
    mean_sq = jnp.mean(hidden * hidden, axis=-1, keepdims=True)
    return (hidden * lax.rsqrt(mean_sq + NORM_EPS) * (1.0 + scale)).astype(BF16)


def layer_kernel(
    n_dev, part_hbm, cos_ref, sin_ref, pcol_ref, prow_ref, wq_hbm, wk_hbm, wv_hbm, wo_hbm, wg_hbm, wu_hbm, wd_hbm,
    g1_ref, g2_ref, g3_ref, g4_ref, out_ref,
    part, wqkv, wo, wg, wu, wd, acts, own, give, take, ring_out, ring_in, q_buf, k_buf, v_buf, o_buf, h_buf, e_own, x_own,
    part_sem, w_sem, ag_s, ag_r, agd_s, agd_r, rs_s, rs_r, rsd_s, rsd_r,
):
    chips = n_dev // 2
    rows = e_own.shape[0]
    piece = rows // PIECES
    dim = e_own.shape[1]
    n_q, head = q_buf.shape[1], q_buf.shape[3]
    ffn = h_buf.shape[1]

    me = lax.axis_index("tp")
    chip, core = lax.div(me, 2), lax.rem(me, 2)
    step = 1 - 2 * core
    partner = {"tp": me + step}
    ahead = {"tp": 2 * lax.rem(chip + step + chips, chips) + core}
    behind = {"tp": 2 * lax.rem(chip - step + chips, chips) + core}

    def mine(s):
        return 2 * lax.rem(chip - step * s + 2 * chips, chips) + core

    def theirs(s):
        return 2 * lax.rem(chip + step * s + 2 * chips, chips) + 1 - core

    def sub(j):
        return pl.ds(pl.multiple_of(j * piece, piece), piece)

    def block_rows(b):
        return pl.ds(pl.multiple_of(b * rows, rows), rows)

    def part_copy(b, i):
        return pltpu.make_async_copy(part_hbm.at[b], part.at[b], part_sem.at[i])

    order = []
    for s in range(chips):
        order.append(theirs(s + 1))
        order.append(mine(s + 1))
    for i, b in enumerate(order):
        part_copy(b, i).start()
    w_copies = [pltpu.make_async_copy(wq_hbm.at[h], wqkv.at[:, pl.ds(h * head, head)], w_sem.at[h]) for h in range(n_q)]
    w_copies.append(pltpu.make_async_copy(wk_hbm, wqkv.at[:, pl.ds(n_q * head, head)], w_sem.at[n_q]))
    w_copies.append(pltpu.make_async_copy(wv_hbm, wqkv.at[:, pl.ds((n_q + 1) * head, head)], w_sem.at[n_q + 1]))
    n_qkv = len(w_copies)
    for i, (src, dst) in enumerate(((wo_hbm, wo), (wg_hbm, wg), (wu_hbm, wu), (wd_hbm, wd))):
        w_copies.append(pltpu.make_async_copy(src, dst, w_sem.at[n_qkv + i]))
    for copy in w_copies:
        copy.start()

    barrier = pltpu.get_barrier_semaphore()
    for peer in (partner, ahead, behind):
        pl.semaphore_signal(barrier, inc=1, device_id=peer, device_id_type=MESH)
    pl.semaphore_wait(barrier, 3)

    def remote(src, dst, send, recv, peer):
        return pltpu.make_async_remote_copy(
            src_ref=src, dst_ref=dst, send_sem=send, recv_sem=recv, device_id=peer, device_id_type=MESH
        )

    def ag_ring(buf, s, j, b):
        return remote(buf.at[b, sub(j)], buf.at[b, sub(j)], ag_s.at[s, j], ag_r.at[s, j], ahead)

    def ag_chip(buf, s, j, b):
        return remote(buf.at[b, sub(j)], buf.at[b, sub(j)], agd_s.at[s, j], agd_r.at[s, j], partner)

    def ag_begin(buf, j):
        ag_ring(buf, 0, j, mine(0)).start()
        ag_chip(buf, 0, j, mine(0)).start()

    def ag_forward(buf, s, j):
        ag_ring(buf, s - 1, j, mine(s)).wait_recv()
        if s < chips - 1:
            ag_ring(buf, s, j, mine(s)).start()
        ag_chip(buf, s, j, mine(s)).start()

    def ag_join(buf, s):
        def body(j, _):
            ag_chip(buf, s, j, theirs(s)).wait_recv()
            return 0
        lax.fori_loop(0, PIECES, body, 0)

    def ag_drain(buf):
        def body(j, _):
            for s in range(chips):
                if s < chips - 1:
                    ag_ring(buf, s, j, mine(s)).wait_send()
                ag_chip(buf, s, j, mine(s)).wait_send()
            return 0
        lax.fori_loop(0, PIECES, body, 0)

    def rs_chip(s, src):
        return remote(src, take.at[s], rsd_s.at[s], rsd_r.at[s], partner)

    def rs_ring(r, t, j):
        slot = (r % 2) * (chips - 1) + t
        return remote(ring_out.at[t, sub(j)], ring_in.at[slot, sub(j)], rs_s.at[t, j], rs_r.at[slot, j], ahead)

    def rs_sum(r, t, j, own_ref):
        s = (t + 1) % chips
        total = own_ref[sub(j), :].astype(F32) + take[s, sub(j), :].astype(F32)
        if t > 0:
            rs_ring(r, t - 1, j).wait_recv()
            total = total + ring_in[(r % 2) * (chips - 1) + t - 1, sub(j), :].astype(F32)
        return total.astype(BF16)

    def rs_stage(r, t, own_ref, src):
        s = (t + 1) % chips
        rs_chip(s, src).wait_recv()

        def body(j, _):
            ring_out[t, sub(j), :] = rs_sum(r, t, j, own_ref)
            rs_ring(r, t, j).start()
            return 0
        lax.fori_loop(0, PIECES, body, 0)

    def rs_last(r, own_ref, src, finish):
        rs_chip(0, src).wait_recv()

        def body(j, _):
            finish(j, rs_sum(r, chips - 1, j, own_ref))
            return 0
        lax.fori_loop(0, PIECES, body, 0)

    def rs_drain(r, src):
        def body(j, _):
            for t in range(chips - 1):
                rs_ring(r, t, j).wait_send()
            return 0
        lax.fori_loop(0, PIECES, body, 0)
        for s in range(chips):
            rs_chip(s, src(s)).wait_send()

    for s in range(chips):
        b = theirs(s + 1)
        part_copy(b, 2 * s).wait()
        rs_chip((s + 1) % chips, part.at[b]).start()
    for s in range(chips):
        part_copy(mine(s + 1), 2 * s + 1).wait()

    def emb_part(s):
        return part.at[theirs(s)]

    for t in range(chips - 1):
        rs_stage(0, t, part.at[mine(t + 1)], emb_part(t + 1))

    def emb_finish(j, e):
        e_own[sub(j), :] = e
        acts[mine(0), sub(j), :] = norm_rows(e.astype(F32), g1_ref[...])
        ag_begin(acts, j)

    rs_last(0, part.at[mine(0)], emb_part(0), emb_finish)
    rs_drain(0, emb_part)

    for copy in w_copies[:n_qkv]:
        copy.wait()

    def pair(ref, s):
        return jnp.concatenate([ref[mine(s)], ref[theirs(s)]], axis=0)

    def pair_rows(ref, s):
        return jnp.concatenate([ref[block_rows(mine(s)), :], ref[block_rows(theirs(s)), :]], axis=0)

    def rope(states, cos, sin):
        return states * cos + pltpu.roll(states, head // 2, axis=1) * sin

    def project(s):
        x = pair(acts, s)
        cos, sin = pair_rows(cos_ref, s), pair_rows(sin_ref, s)
        for start in range(0, n_q + 2, 2):
            width = min(2, n_q + 2 - start)
            res = jnp.dot(x, wqkv[:, start * head : (start + width) * head], preferred_element_type=F32)
            for i in range(width):
                h, states = start + i, res[:, i * head : (i + 1) * head]
                if h < n_q:
                    q_buf[s, h] = (rope(states, cos, sin) * QUERY_SCALE).astype(BF16)
                else:
                    val = (rope(states, cos, sin) if h == n_q else states).astype(BF16)
                    dst = k_buf if h == n_q else v_buf
                    dst[block_rows(mine(s)), :] = val[:rows]
                    dst[block_rows(theirs(s)), :] = val[rows:]

    for s in range(chips):
        if s < chips - 1:
            def body(j, _):
                ag_forward(acts, s + 1, j)
                return 0
        ag_join(acts, s)
        project(s)
        if s < chips - 1:
            lax.fori_loop(0, PIECES, body, 0)

    def attend(s):
        key_pos = prow_ref[...]
        offset = pair_rows(pcol_ref, s) - key_pos
        keep = (offset >= 0) & (offset < WINDOW)

        for h in range(n_q):
            scores = lax.dot_general(q_buf[s, h], k_buf[...], NT, preferred_element_type=F32)
            capped = SOFT_CAP * jnp.tanh(scores * (1.0 / SOFT_CAP))
            weight = jnp.where(keep, jnp.exp(capped), 0.0)
            total = jnp.sum(weight, axis=-1, keepdims=True)
            probs = (weight * (1.0 / total)).astype(BF16)
            mix = jnp.dot(probs, v_buf[...], preferred_element_type=F32)
            o_buf[:, h * head : (h + 1) * head] = mix.astype(BF16)

    def spread(s, lhs_ref, w_ref, width):
        @pl.loop(0, dim // width)
        def _(i):
            cols = pl.ds(pl.multiple_of(i * width, width), width)
            res = jnp.dot(lhs_ref[...], w_ref[:, cols], preferred_element_type=F32).astype(BF16)
            own[s, :, cols] = res[:rows]
            give[s, :, cols] = res[rows:]
        rs_chip(s, give.at[s]).start()

    w_copies[n_qkv].wait()
    for i in range(chips):
        s = (i + 1) % chips
        attend(s)
        spread(s, o_buf, wo, 512)
        if i > 0:
            rs_stage(1, i - 1, own.at[i], give.at[i])
    ag_drain(acts)

    def att_finish(j, y):
        x1 = (e_own[sub(j), :].astype(F32) + norm_rows(y.astype(F32), g2_ref[...]).astype(F32)).astype(BF16)
        x_own[sub(j), :] = x1
        part[mine(0), sub(j), :] = norm_rows(x1.astype(F32), g3_ref[...])
        ag_begin(part, j)

    rs_last(1, own.at[0], give.at[0], att_finish)
    rs_drain(1, lambda s: give.at[s])

    for copy in w_copies[n_qkv + 1 :]:
        copy.wait()
    tile = ffn // PIECES

    def gate_up(s, i):
        x = pair(part, s)
        cols = pl.ds(i * tile, tile)
        gate = jnp.dot(x, wg[:, cols], preferred_element_type=F32)
        up = jnp.dot(x, wu[:, cols], preferred_element_type=F32)
        h_buf[:, cols] = (jax.nn.gelu(gate, approximate=True) * up).astype(BF16)

    for s in range(chips):
        ag_join(part, s)
        if s == chips - 2:
            rs_stage(2, 0, own.at[1], give.at[1])
        for i in range(PIECES):
            gate_up(s, i)
            if s < chips - 1:
                ag_forward(part, s + 1, i)
        spread(s, h_buf, wd, 512)
    for t in range(1, chips - 1):
        rs_stage(2, t, own.at[t + 1], give.at[t + 1])
    ag_drain(part)

    def ffn_finish(j, z):
        out = x_own[sub(j), :].astype(F32) + norm_rows(z.astype(F32), g4_ref[...]).astype(F32)
        out_ref[sub(j), :] = out.astype(BF16)

    rs_last(2, own.at[0], give.at[0], ffn_finish)
    rs_drain(2, lambda s: give.at[s])


def decoder_layer(n_dev, part, positions, w_query, w_key, w_value, w_out, w_gate, w_up, w_down, g1, g2, g3, g4):
    seq_len = positions.shape[1]
    dim, n_q, head = w_query.shape
    ffn = w_gate.shape[1]
    chips, rows = n_dev // 2, seq_len // n_dev
    half = head // 2
    inv_freq = ROPE_BASE ** (-2.0 * jnp.arange(half, dtype=F32) / head)
    angles = positions[0].astype(F32)[:, None] * inv_freq
    cos_tab, sin_tab = jnp.cos(angles), jnp.sin(angles)
    cos2 = jnp.concatenate([cos_tab, cos_tab], axis=1)
    sin2 = jnp.concatenate([-sin_tab, sin_tab], axis=1)
    vmem = pl.BlockSpec(memory_space=pltpu.VMEM)
    hbm = pl.BlockSpec(memory_space=pl.ANY)
    block = (rows, dim)
    dma = pltpu.SemaphoreType.DMA
    return pl.pallas_call(
        functools.partial(layer_kernel, n_dev),
        name="layer",
        out_shape=jax.ShapeDtypeStruct((rows, dim), BF16),
        in_specs=[hbm] + [vmem] * 4 + [hbm] * 7 + [vmem] * 4,
        out_specs=vmem,
        scratch_shapes=[
            pltpu.VMEM((n_dev,) + block, BF16),
            pltpu.VMEM((dim, (n_q + 2) * head), BF16),
            pltpu.VMEM((n_q * head, dim), BF16),
            pltpu.VMEM((dim, ffn), BF16),
            pltpu.VMEM((dim, ffn), BF16),
            pltpu.VMEM((ffn, dim), BF16),
            pltpu.VMEM((n_dev,) + block, BF16),
            pltpu.VMEM((chips,) + block, BF16),
            pltpu.VMEM((chips,) + block, BF16),
            pltpu.VMEM((chips,) + block, BF16),
            pltpu.VMEM((chips - 1,) + block, BF16),
            pltpu.VMEM((2 * (chips - 1),) + block, BF16),
            pltpu.VMEM((chips, n_q, 2 * rows, head), BF16),
            pltpu.VMEM((seq_len, head), BF16),
            pltpu.VMEM((seq_len, head), BF16),
            pltpu.VMEM((2 * rows, n_q * head), BF16),
            pltpu.VMEM((2 * rows, ffn), BF16),
            pltpu.VMEM(block, BF16),
            pltpu.VMEM(block, BF16),
            dma((n_dev,)),
            dma((n_q + 6,)),
            dma((chips - 1, PIECES)),
            dma((chips - 1, PIECES)),
            dma((chips, PIECES)),
            dma((chips, PIECES)),
            dma((chips - 1, PIECES)),
            dma((2 * (chips - 1), PIECES)),
            dma((chips,)),
            dma((chips,)),
        ],
        compiler_params=pltpu.CompilerParams(collective_id=0, has_side_effects=True, vmem_limit_bytes=58 * 1024 * 1024),
    )(
        part.reshape((n_dev,) + block), cos2, sin2, positions.reshape(seq_len, 1), positions.reshape(1, seq_len),
        w_query.transpose(1, 0, 2), w_key.reshape(dim, head), w_value.reshape(dim, head), w_out.reshape(n_q * head, dim),
        w_gate, w_up, w_down, g1.reshape(1, dim), g2.reshape(1, dim), g3.reshape(1, dim), g4.reshape(1, dim),
    )


def solution(mesh):
    n_dev = mesh.shape["tp"]
    in_specs = (P("dp", None), P("dp", None), P("tp", None), P(None, "tp", None), P(None, "tp", None), P(None, "tp", None), P("tp", None, None), P(None, "tp"), P(None, "tp"), P("tp", None), P(None), P(None), P(None), P(None))

    def device_step(tokens, positions, embed_block, *weights):
        dev_rank = lax.axis_index("tp")
        vocab_local, model_dim = embed_block.shape
        local_ids = tokens[0] - dev_rank * vocab_local
        in_block = (local_ids >= 0) & (local_ids < vocab_local)
        looked = jnp.take(embed_block, jnp.clip(local_ids, 0, vocab_local - 1), axis=0)
        normalizer = jnp.sqrt(jnp.float32(model_dim)).astype(BF16)
        part = jnp.where(in_block[:, None], looked * normalizer, jnp.zeros((), BF16))
        return decoder_layer(n_dev, part, positions, *weights)[None]

    return jax.shard_map(device_step, mesh=mesh, in_specs=in_specs, out_specs=P("dp", "tp", None), check_vma=False)
```

```python
import functools

import jax
import jax.numpy as jnp
from jax import lax
from jax.experimental import pallas as pl
from jax.experimental.pallas import tpu as pltpu
from jax.sharding import PartitionSpec as P

WINDOW = 4096
QUERY_SCALE = 256.0 ** -0.5
SOFT_CAP = 50.0
NORM_EPS = 1e-6
ROPE_BASE = 10000.0
MESH = pl.DeviceIdType.MESH
BF16 = jnp.bfloat16
F32 = jnp.float32
PIECES = 4
TOKENS = 128
UNROLL = 8
NT = (((1,), (1,)), ((), ()))


def norm_rows(hidden, scale):
    mean_sq = jnp.mean(hidden * hidden, axis=-1, keepdims=True)
    return (hidden * lax.rsqrt(mean_sq + NORM_EPS) * (1.0 + scale)).astype(BF16)


def layer_kernel(
    n_dev, part, freq_ref, prow_ref, wq_hbm, wk_hbm, wv_hbm, wo_hbm, wg_hbm, wu_hbm, wd_hbm,
    g1_ref, g2_ref, g3_ref, g4_ref, out_ref,
    wqkv, wo, wg, wu, wd, acts, acts2, cos_ref, sin_ref, pcol_ref, own, give, take, ring_out, ring_in, q_buf, k_buf, v_buf, o_buf, h_buf, e_own, x_own,
    w_sem, ag_s, ag_r, agd_s, agd_r, rs_s, rs_r, rsd_s, rsd_r,
):
    chips = n_dev // 2
    rows = e_own.shape[0]
    piece = rows // PIECES
    dim = e_own.shape[1]
    n_q, head = q_buf.shape[1], q_buf.shape[3]
    ffn = h_buf.shape[1]

    me = lax.axis_index("tp")
    chip, core = lax.div(me, 2), lax.rem(me, 2)
    step = 1 - 2 * core
    partner = {"tp": me + step}
    ahead = {"tp": 2 * lax.rem(chip + step + chips, chips) + core}
    behind = {"tp": 2 * lax.rem(chip - step + chips, chips) + core}

    def mine(s):
        return 2 * lax.rem(chip - step * s + 2 * chips, chips) + core

    def theirs(s):
        return 2 * lax.rem(chip + step * s + 2 * chips, chips) + 1 - core

    def sub(j):
        return pl.ds(pl.multiple_of(j * piece, piece), piece)

    def block_rows(b):
        return pl.ds(pl.multiple_of(b * rows, rows), rows)

    w_copies = [pltpu.make_async_copy(wq_hbm.at[h], wqkv.at[:, pl.ds(h * head, head)], w_sem.at[h]) for h in range(n_q)]
    w_copies.append(pltpu.make_async_copy(wk_hbm, wqkv.at[:, pl.ds(n_q * head, head)], w_sem.at[n_q]))
    w_copies.append(pltpu.make_async_copy(wv_hbm, wqkv.at[:, pl.ds((n_q + 1) * head, head)], w_sem.at[n_q + 1]))
    n_qkv = len(w_copies)
    for i, (src, dst) in enumerate(((wo_hbm, wo), (wg_hbm, wg), (wu_hbm, wu), (wd_hbm, wd))):
        w_copies.append(pltpu.make_async_copy(src, dst, w_sem.at[n_qkv + i]))
    for copy in w_copies:
        copy.start()

    barrier = pltpu.get_barrier_semaphore()
    for peer in (partner, ahead, behind):
        pl.semaphore_signal(barrier, inc=1, device_id=peer, device_id_type=MESH)
    pl.semaphore_wait(barrier, 3)

    def remote(src, dst, send, recv, peer):
        return pltpu.make_async_remote_copy(
            src_ref=src, dst_ref=dst, send_sem=send, recv_sem=recv, device_id=peer, device_id_type=MESH
        )

    def ag_ring(buf, s, j, b):
        return remote(buf.at[b, sub(j)], buf.at[b, sub(j)], ag_s.at[s, j], ag_r.at[s, j], ahead)

    def ag_chip(buf, s, j, b):
        return remote(buf.at[b, sub(j)], buf.at[b, sub(j)], agd_s.at[s, j], agd_r.at[s, j], partner)

    def ag_begin(buf, j):
        ag_ring(buf, 0, j, mine(0)).start()
        ag_chip(buf, 0, j, mine(0)).start()

    def ag_forward(buf, s, j):
        ag_ring(buf, s - 1, j, mine(s)).wait_recv()
        if s < chips - 1:
            ag_ring(buf, s, j, mine(s)).start()
        ag_chip(buf, s, j, mine(s)).start()

    def ag_join(buf, s):
        def body(j, _):
            ag_chip(buf, s, j, theirs(s)).wait_recv()
            return 0
        lax.fori_loop(0, PIECES, body, 0)

    def ag_drain(buf):
        def body(j, _):
            for s in range(chips):
                if s < chips - 1:
                    ag_ring(buf, s, j, mine(s)).wait_send()
                ag_chip(buf, s, j, mine(s)).wait_send()
            return 0
        lax.fori_loop(0, PIECES, body, 0)

    def rs_chip(s, src):
        return remote(src, take.at[s], rsd_s.at[s], rsd_r.at[s], partner)

    def rs_ring(r, t, j):
        slot = (r % 2) * (chips - 1) + t
        return remote(ring_out.at[t, sub(j)], ring_in.at[slot, sub(j)], rs_s.at[t, j], rs_r.at[slot, j], ahead)

    def rs_sum(r, t, j, own_ref):
        s = (t + 1) % chips
        total = own_ref[sub(j), :].astype(F32) + take[s, sub(j), :].astype(F32)
        if t > 0:
            rs_ring(r, t - 1, j).wait_recv()
            total = total + ring_in[(r % 2) * (chips - 1) + t - 1, sub(j), :].astype(F32)
        return total.astype(BF16)

    def rs_stage(r, t, own_ref, src):
        s = (t + 1) % chips
        rs_chip(s, src).wait_recv()

        def body(j, _):
            ring_out[t, sub(j), :] = rs_sum(r, t, j, own_ref)
            rs_ring(r, t, j).start()
            return 0
        lax.fori_loop(0, PIECES, body, 0)

    def rs_last(r, own_ref, src, finish):
        rs_chip(0, src).wait_recv()

        def body(j, _):
            finish(j, rs_sum(r, chips - 1, j, own_ref))
            return 0
        lax.fori_loop(0, PIECES, body, 0)

    def rs_drain(r, src):
        def body(j, _):
            for t in range(chips - 1):
                rs_ring(r, t, j).wait_send()
            return 0
        lax.fori_loop(0, PIECES, body, 0)
        for s in range(chips):
            rs_chip(s, src(s)).wait_send()

    def emb_part(s):
        return part.at[theirs(s)]

    for s in range(chips):
        rs_chip((s + 1) % chips, emb_part(s + 1)).start()
    for t in range(chips - 1):
        rs_stage(0, t, part.at[mine(t + 1)], emb_part(t + 1))
        if t == 0:
            pcol_ref[...] = jnp.transpose(jnp.broadcast_to(prow_ref[...], (head, prow_ref.shape[1])))
            angles = pcol_ref[...].astype(F32) * freq_ref[...]
            lane = lax.broadcasted_iota(jnp.int32, angles.shape, 1)
            cos_ref[...] = jnp.cos(angles)
            sin = jnp.sin(angles)
            sin_ref[...] = jnp.where(lane < head // 2, -sin, sin)

    def emb_finish(j, e):
        e_own[sub(j), :] = e
        acts[mine(0), sub(j), :] = norm_rows(e.astype(F32), g1_ref[...])
        ag_begin(acts, j)

    rs_last(0, part.at[mine(0)], emb_part(0), emb_finish)
    rs_drain(0, emb_part)

    for copy in w_copies[:n_qkv]:
        copy.wait()

    def pair(ref, s):
        return jnp.concatenate([ref[mine(s)], ref[theirs(s)]], axis=0)

    def pair_rows(ref, s):
        return jnp.concatenate([ref[block_rows(mine(s)), :], ref[block_rows(theirs(s)), :]], axis=0)

    def rope(states, cos, sin):
        return states * cos + pltpu.roll(states, head // 2, axis=1) * sin

    def project(s):
        x = pair(acts, s)
        cos, sin = pair_rows(cos_ref, s), pair_rows(sin_ref, s)
        for start in range(0, n_q + 2, 2):
            width = min(2, n_q + 2 - start)
            res = jnp.dot(x, wqkv[:, start * head : (start + width) * head], preferred_element_type=F32)
            for i in range(width):
                h, states = start + i, res[:, i * head : (i + 1) * head]
                if h < n_q:
                    q_buf[s, h] = (rope(states, cos, sin) * QUERY_SCALE).astype(BF16)
                else:
                    val = (rope(states, cos, sin) if h == n_q else states).astype(BF16)
                    dst = k_buf if h == n_q else v_buf
                    dst[block_rows(mine(s)), :] = val[:rows]
                    dst[block_rows(theirs(s)), :] = val[rows:]

    for s in range(chips):
        if s < chips - 1:
            def body(j, _):
                ag_forward(acts, s + 1, j)
                return 0
        ag_join(acts, s)
        project(s)
        if s < chips - 1:
            lax.fori_loop(0, PIECES, body, 0)

    def attend(s):
        key_pos = prow_ref[...]
        offset = pair_rows(pcol_ref, s)[:, 0:1] - key_pos
        keep = (offset >= 0) & (offset < WINDOW)

        for h in range(n_q):
            scores = lax.dot_general(q_buf[s, h], k_buf[...], NT, preferred_element_type=F32)
            capped = SOFT_CAP * jnp.tanh(scores * (1.0 / SOFT_CAP))
            weight = jnp.where(keep, jnp.exp(capped), 0.0)
            total = jnp.sum(weight, axis=-1, keepdims=True)
            probs = (weight * (1.0 / total)).astype(BF16)
            mix = jnp.dot(probs, v_buf[...], preferred_element_type=F32)
            o_buf[:, h * head : (h + 1) * head] = mix.astype(BF16)

    def spread(s, lhs_ref, w_ref, width):
        @pl.loop(0, dim // width)
        def _(i):
            cols = pl.ds(pl.multiple_of(i * width, width), width)
            res = jnp.dot(lhs_ref[...], w_ref[:, cols], preferred_element_type=F32).astype(BF16)
            own[s, :, cols] = res[:rows]
            give[s, :, cols] = res[rows:]
        rs_chip(s, give.at[s]).start()

    w_copies[n_qkv].wait()
    for i in range(chips):
        s = (i + 1) % chips
        attend(s)
        spread(s, o_buf, wo, 512)
        if i > 0:
            rs_stage(1, i - 1, own.at[i], give.at[i])
    ag_drain(acts)

    def att_finish(j, y):
        x1 = (e_own[sub(j), :].astype(F32) + norm_rows(y.astype(F32), g2_ref[...]).astype(F32)).astype(BF16)
        x_own[sub(j), :] = x1
        acts2[mine(0), sub(j), :] = norm_rows(x1.astype(F32), g3_ref[...])
        ag_begin(acts2, j)

    rs_last(1, own.at[0], give.at[0], att_finish)
    rs_drain(1, lambda s: give.at[s])

    for copy in w_copies[n_qkv + 1 :]:
        copy.wait()
    tile = ffn // PIECES

    def gate_up(s, i):
        x = pair(acts2, s)
        cols = pl.ds(i * tile, tile)
        gate = jnp.dot(x, wg[:, cols], preferred_element_type=F32)
        up = jnp.dot(x, wu[:, cols], preferred_element_type=F32)
        h_buf[:, cols] = (jax.nn.gelu(gate, approximate=True) * up).astype(BF16)

    for s in range(chips):
        ag_join(acts2, s)
        if s == chips - 2:
            rs_stage(2, 0, own.at[1], give.at[1])
        for i in range(PIECES):
            gate_up(s, i)
            if s < chips - 1:
                ag_forward(acts2, s + 1, i)
        spread(s, h_buf, wd, 512)
    for t in range(1, chips - 1):
        rs_stage(2, t, own.at[t + 1], give.at[t + 1])
    ag_drain(acts2)

    def ffn_finish(j, z):
        out = x_own[sub(j), :].astype(F32) + norm_rows(z.astype(F32), g4_ref[...]).astype(F32)
        out_ref[sub(j), :] = out.astype(BF16)

    rs_last(2, own.at[0], give.at[0], ffn_finish)
    rs_drain(2, lambda s: give.at[s])


def lookup_kernel(n_dev, tok_ref, tokrow_ref, table_hbm, out_ref, slots, tokcol, counts, sem):
    vocab, dim = table_hbm.shape
    seq_len = out_ref.shape[0]
    base = lax.axis_index("tp") * vocab
    n_blocks = seq_len // TOKENS
    unit = 8

    for g in range(n_blocks):
        def issue(i, count):
            for u in range(UNROLL):
                local = tok_ref[0, g * TOKENS + i * UNROLL + u] - base
                inside = (local >= 0) & (local < vocab)

                @pl.when(inside)
                def _():
                    src = pl.multiple_of(lax.shift_left(lax.shift_right_logical(local, 3), 3), unit)
                    dst = pl.multiple_of((g * TOKENS + count) * unit, unit)
                    pltpu.make_async_copy(table_hbm.at[pl.ds(src, unit), :], slots.at[pl.ds(dst, unit), :], sem.at[g]).start()
                count = count + jnp.where(inside, 1, 0)
            return count
        counts[g] = lax.fori_loop(0, TOKENS // UNROLL, issue, jnp.int32(0))

    tokcol[...] = jnp.transpose(jnp.broadcast_to(tokrow_ref[...], (TOKENS, seq_len)))
    scale = jnp.sqrt(jnp.float32(dim)).astype(BF16).astype(F32)
    depth = 256
    before = lax.broadcasted_iota(jnp.int32, (TOKENS, TOKENS), 1) < lax.broadcasted_iota(jnp.int32, (TOKENS, TOKENS), 0)
    col = lax.broadcasted_iota(jnp.int32, (TOKENS, depth), 1)
    slot_row = lax.broadcasted_iota(jnp.int32, (depth, dim), 0)

    for g in range(n_blocks):
        count = counts[g]

        def wait(i, _):
            pltpu.make_async_copy(table_hbm.at[pl.ds(0, unit), :], slots.at[pl.ds(0, unit), :], sem.at[g]).wait()
            return 0
        lax.fori_loop(0, count, wait, 0)
        span = slice(g * TOKENS, (g + 1) * TOKENS)
        row = tokrow_ref[:, span] - base
        row_in = ((row >= 0) & (row < vocab)).astype(F32)
        place = jnp.sum(jnp.where(before, row_in, 0.0), axis=1, keepdims=True).astype(jnp.int32)
        local = tokcol[span, 0:1] - base
        inside = (local >= 0) & (local < vocab)
        want = jnp.where(inside, place * unit + (local & 7), -1)

        def pick(kt):
            first = pl.multiple_of((g * TOKENS * unit) + kt * depth, depth)
            hot = (col + kt * depth == want).astype(F32).astype(BF16)
            held = jnp.where(slot_row + kt * depth < count * unit, slots[pl.ds(first, depth), :], jnp.zeros((), BF16))
            return (jnp.dot(hot, held, preferred_element_type=F32) * scale).astype(BF16)

        out_ref[span, :] = pick(0)

        def more(kt, _):
            out_ref[span, :] = out_ref[span, :] + pick(kt)
            return 0
        lax.fori_loop(1, lax.div(count * unit + depth - 1, depth), more, 0)


def lookup(n_dev, tokens, embed_block):
    seq_len, dim = tokens.shape[1], embed_block.shape[1]
    return pl.pallas_call(
        functools.partial(lookup_kernel, n_dev),
        name="lookup",
        out_shape=jax.ShapeDtypeStruct((seq_len, dim), BF16),
        in_specs=[pl.BlockSpec(memory_space=pltpu.SMEM), pl.BlockSpec(memory_space=pltpu.VMEM), pl.BlockSpec(memory_space=pl.ANY)],
        out_specs=pl.BlockSpec(memory_space=pltpu.VMEM),
        scratch_shapes=[
            pltpu.VMEM((8 * seq_len, dim), BF16),
            pltpu.VMEM((seq_len, TOKENS), jnp.int32),
            pltpu.SMEM((seq_len // TOKENS,), jnp.int32),
            pltpu.SemaphoreType.DMA((seq_len // TOKENS,)),
        ],
        compiler_params=pltpu.CompilerParams(vmem_limit_bytes=48 * 1024 * 1024),
    )(tokens, tokens, embed_block)


def decoder_layer(n_dev, part, positions, w_query, w_key, w_value, w_out, w_gate, w_up, w_down, g1, g2, g3, g4):
    seq_len = positions.shape[1]
    dim, n_q, head = w_query.shape
    ffn = w_gate.shape[1]
    chips, rows = n_dev // 2, seq_len // n_dev
    inv_freq = ROPE_BASE ** (-2.0 * jnp.arange(head // 2, dtype=F32) / head)
    freq = jnp.concatenate([inv_freq, inv_freq])[None, :]
    vmem = pl.BlockSpec(memory_space=pltpu.VMEM)
    hbm = pl.BlockSpec(memory_space=pltpu.HBM)
    block = (rows, dim)
    dma = pltpu.SemaphoreType.DMA
    weights = (
        w_query.transpose(1, 0, 2), w_key.reshape(dim, head), w_value.reshape(dim, head), w_out.reshape(n_q * head, dim),
        w_gate, w_up, w_down,
    )
    weights = [pltpu.with_memory_space_constraint(w, pltpu.HBM) for w in weights]
    return pl.pallas_call(
        functools.partial(layer_kernel, n_dev),
        name="layer",
        out_shape=jax.ShapeDtypeStruct((rows, dim), BF16),
        in_specs=[vmem] * 3 + [hbm] * 7 + [vmem] * 4,
        out_specs=vmem,
        scratch_shapes=[
            pltpu.VMEM((dim, (n_q + 2) * head), BF16),
            pltpu.VMEM((n_q * head, dim), BF16),
            pltpu.VMEM((dim, ffn), BF16),
            pltpu.VMEM((dim, ffn), BF16),
            pltpu.VMEM((ffn, dim), BF16),
            pltpu.VMEM((n_dev,) + block, BF16),
            pltpu.VMEM((n_dev,) + block, BF16),
            pltpu.VMEM((seq_len, head), F32),
            pltpu.VMEM((seq_len, head), F32),
            pltpu.VMEM((seq_len, head), jnp.int32),
            pltpu.VMEM((chips,) + block, BF16),
            pltpu.VMEM((chips,) + block, BF16),
            pltpu.VMEM((chips,) + block, BF16),
            pltpu.VMEM((chips - 1,) + block, BF16),
            pltpu.VMEM((2 * (chips - 1),) + block, BF16),
            pltpu.VMEM((chips, n_q, 2 * rows, head), BF16),
            pltpu.VMEM((seq_len, head), BF16),
            pltpu.VMEM((seq_len, head), BF16),
            pltpu.VMEM((2 * rows, n_q * head), BF16),
            pltpu.VMEM((2 * rows, ffn), BF16),
            pltpu.VMEM(block, BF16),
            pltpu.VMEM(block, BF16),
            dma((n_q + 6,)),
            dma((chips - 1, PIECES)),
            dma((chips - 1, PIECES)),
            dma((chips, PIECES)),
            dma((chips, PIECES)),
            dma((chips - 1, PIECES)),
            dma((2 * (chips - 1), PIECES)),
            dma((chips,)),
            dma((chips,)),
        ],
        compiler_params=pltpu.CompilerParams(collective_id=0, has_side_effects=True, vmem_limit_bytes=46 * 1024 * 1024),
    )(
        pltpu.with_memory_space_constraint(part.reshape((n_dev,) + block), pltpu.VMEM), freq, positions, *weights, g1.reshape(1, dim), g2.reshape(1, dim), g3.reshape(1, dim), g4.reshape(1, dim),
    )


def solution(mesh):
    n_dev = mesh.shape["tp"]
    in_specs = (P("dp", None), P("dp", None), P("tp", None), P(None, "tp", None), P(None, "tp", None), P(None, "tp", None), P("tp", None, None), P(None, "tp"), P(None, "tp"), P("tp", None), P(None), P(None), P(None), P(None))

    def device_step(tokens, positions, embed_block, *weights):
        part = lookup(n_dev, tokens, embed_block)
        return decoder_layer(n_dev, part, positions, *weights)[None]

    return jax.shard_map(device_step, mesh=mesh, in_specs=in_specs, out_specs=P("dp", "tp", None), check_vma=False)
```

```python
import functools

import jax
import jax.numpy as jnp
from jax import lax
from jax.experimental import pallas as pl
from jax.experimental.pallas import tpu as pltpu
from jax.sharding import PartitionSpec as P

WINDOW = 4096
QUERY_SCALE = 256.0 ** -0.5
SOFT_CAP = 50.0
NORM_EPS = 1e-6
ROPE_BASE = 10000.0
MESH = pl.DeviceIdType.MESH
BF16 = jnp.bfloat16
F32 = jnp.float32
PIECES = 4
SPREAD = 3072
FFN_TILE = 512
TOKENS = 128
UNROLL = 8
NT = (((1,), (1,)), ((), ()))


def norm_rows(hidden, scale):
    mean_sq = jnp.mean(hidden * hidden, axis=-1, keepdims=True)
    return (hidden * lax.rsqrt(mean_sq + NORM_EPS) * (1.0 + scale)).astype(BF16)


def layer_kernel(
    n_dev, part, freq_ref, prow_ref, wq_hbm, wk_hbm, wv_hbm, wo_hbm, wg_hbm, wu_hbm, wd_hbm,
    g1_ref, g2_ref, g3_ref, g4_ref, out_ref,
    wqkv, wo, wg, wu, wd, acts, acts2, cos_ref, sin_ref, pcol_ref, own, give, take, ring_out, ring_in, q_buf, k_buf, v_buf, o_buf, h_buf, e_own, x_own,
    w_sem, ag_s, ag_r, agd_s, agd_r, rs_s, rs_r, rsd_s, rsd_r,
):
    chips = n_dev // 2
    rows = e_own.shape[0]
    piece = rows // PIECES
    dim = e_own.shape[1]
    n_q, head = q_buf.shape[1], q_buf.shape[3]
    ffn = h_buf.shape[1]

    me = lax.axis_index("tp")
    chip, core = lax.div(me, 2), lax.rem(me, 2)
    step = 1 - 2 * core
    partner = {"tp": me + step}
    ahead = {"tp": 2 * lax.rem(chip + step + chips, chips) + core}
    behind = {"tp": 2 * lax.rem(chip - step + chips, chips) + core}

    def mine(s):
        return 2 * lax.rem(chip - step * s + 2 * chips, chips) + core

    def theirs(s):
        return 2 * lax.rem(chip + step * s + 2 * chips, chips) + 1 - core

    def sub(j):
        return pl.ds(pl.multiple_of(j * piece, piece), piece)

    def block_rows(b):
        return pl.ds(pl.multiple_of(b * rows, rows), rows)

    w_copies = [pltpu.make_async_copy(wq_hbm.at[h], wqkv.at[:, pl.ds(h * head, head)], w_sem.at[h]) for h in range(n_q)]
    w_copies.append(pltpu.make_async_copy(wk_hbm, wqkv.at[:, pl.ds(n_q * head, head)], w_sem.at[n_q]))
    w_copies.append(pltpu.make_async_copy(wv_hbm, wqkv.at[:, pl.ds((n_q + 1) * head, head)], w_sem.at[n_q + 1]))
    n_qkv = len(w_copies)
    for i, (src, dst) in enumerate(((wo_hbm, wo), (wg_hbm, wg), (wu_hbm, wu), (wd_hbm, wd))):
        w_copies.append(pltpu.make_async_copy(src, dst, w_sem.at[n_qkv + i]))
    for copy in w_copies:
        copy.start()

    barrier = pltpu.get_barrier_semaphore()
    for peer in (partner, ahead, behind):
        pl.semaphore_signal(barrier, inc=1, device_id=peer, device_id_type=MESH)
    pl.semaphore_wait(barrier, 3)

    def remote(src, dst, send, recv, peer):
        return pltpu.make_async_remote_copy(
            src_ref=src, dst_ref=dst, send_sem=send, recv_sem=recv, device_id=peer, device_id_type=MESH
        )

    def ag_ring(buf, s, j, b):
        return remote(buf.at[b, sub(j)], buf.at[b, sub(j)], ag_s.at[s, j], ag_r.at[s, j], ahead)

    def ag_chip(buf, s, j, b):
        return remote(buf.at[b, sub(j)], buf.at[b, sub(j)], agd_s.at[s, j], agd_r.at[s, j], partner)

    def ag_begin(buf, j):
        ag_ring(buf, 0, j, mine(0)).start()
        ag_chip(buf, 0, j, mine(0)).start()

    def ag_forward(buf, s, j):
        ag_ring(buf, s - 1, j, mine(s)).wait_recv()
        if s < chips - 1:
            ag_ring(buf, s, j, mine(s)).start()
        ag_chip(buf, s, j, mine(s)).start()

    def ag_join(buf, s):
        def body(j, _):
            ag_chip(buf, s, j, theirs(s)).wait_recv()
            return 0
        lax.fori_loop(0, PIECES, body, 0)

    def ag_drain(buf):
        def body(j, _):
            for s in range(chips):
                if s < chips - 1:
                    ag_ring(buf, s, j, mine(s)).wait_send()
                ag_chip(buf, s, j, mine(s)).wait_send()
            return 0
        lax.fori_loop(0, PIECES, body, 0)

    def rs_chip_rows(s, j, b):
        return remote(part.at[b, sub(j)], take.at[s, sub(j)], rsd_s.at[s, j], rsd_r.at[s, j], partner)

    def rs_chip_cols(s, i):
        return remote(give.at[s], take.at[s], rsd_s.at[s, i], rsd_r.at[s, i], partner)

    def cols_arrive(s):
        def body(i, _):
            rs_chip_cols(s, i).wait_recv()
            return 0
        lax.fori_loop(0, 1, body, 0)

    def rs_ring(r, t, j):
        slot = (r % 2) * (chips - 1) + t
        return remote(ring_out.at[t, sub(j)], ring_in.at[slot, sub(j)], rs_s.at[t, j], rs_r.at[slot, j], ahead)

    def rs_sum(r, t, j, own_ref):
        s = (t + 1) % chips
        total = own_ref[sub(j), :].astype(F32) + take[s, sub(j), :].astype(F32)
        if t > 0:
            rs_ring(r, t - 1, j).wait_recv()
            total = total + ring_in[(r % 2) * (chips - 1) + t - 1, sub(j), :].astype(F32)
        return total.astype(BF16)

    def rs_piece(r, t, own_ref, j):
        ring_out[t, sub(j), :] = rs_sum(r, t, j, own_ref)
        rs_ring(r, t, j).start()

    def rs_stage(r, t):
        cols_arrive(t + 1)

        def body(j, _):
            rs_piece(r, t, own.at[t + 1], j)
            return 0
        lax.fori_loop(0, PIECES, body, 0)

    def rs_last(r, finish):
        cols_arrive(0)

        def body(j, _):
            finish(j, rs_sum(r, chips - 1, j, own.at[0]))
            return 0
        lax.fori_loop(0, PIECES, body, 0)

    def ring_drain(r):
        def body(j, _):
            for t in range(chips - 1):
                rs_ring(r, t, j).wait_send()
            return 0
        lax.fori_loop(0, PIECES, body, 0)

    def cols_drain():
        def body(i, _):
            for s in range(chips):
                rs_chip_cols(s, i).wait_send()
            return 0
        lax.fori_loop(0, 1, body, 0)

    seq_len = prow_ref.shape[1]
    table_rows = seq_len // ((chips - 2) * PIECES)
    pcol_ref[...] = jnp.transpose(jnp.broadcast_to(prow_ref[...], (head, seq_len)))

    def rotary(i):
        span = pl.ds(pl.multiple_of(i * table_rows, table_rows), table_rows)
        angles = pcol_ref[span, :].astype(F32) * freq_ref[...]
        lane = lax.broadcasted_iota(jnp.int32, angles.shape, 1)
        cos_ref[span, :] = jnp.cos(angles)
        sin = jnp.sin(angles)
        sin_ref[span, :] = jnp.where(lane < head // 2, -sin, sin)

    for s in range(chips):
        def body(j, _):
            rs_chip_rows((s + 1) % chips, j, theirs(s + 1)).start()
            return 0
        lax.fori_loop(0, PIECES, body, 0)
    for t in range(chips - 1):
        def body(j, _):
            rs_chip_rows(t + 1, j, theirs(t + 1)).wait_recv()
            rs_piece(0, t, part.at[mine(t + 1)], j)
            if t < chips - 2:
                rotary(t * PIECES + j)
            return 0
        lax.fori_loop(0, PIECES, body, 0)

    def emb_finish(j, _):
        rs_chip_rows(0, j, theirs(0)).wait_recv()
        e = rs_sum(0, chips - 1, j, part.at[mine(0)])
        e_own[sub(j), :] = e
        acts[mine(0), sub(j), :] = norm_rows(e.astype(F32), g1_ref[...])
        ag_begin(acts, j)
        return 0
    lax.fori_loop(0, PIECES, emb_finish, 0)
    ring_drain(0)

    def emb_drain(j, _):
        for s in range(chips):
            rs_chip_rows(s, j, theirs(s)).wait_send()
        return 0
    lax.fori_loop(0, PIECES, emb_drain, 0)

    for copy in w_copies[:n_qkv]:
        copy.wait()

    def pair(ref, s):
        return jnp.concatenate([ref[mine(s)], ref[theirs(s)]], axis=0)

    def pair_rows(ref, s):
        return jnp.concatenate([ref[block_rows(mine(s)), :], ref[block_rows(theirs(s)), :]], axis=0)

    def rope(states, cos, sin):
        return states * cos + pltpu.roll(states, head // 2, axis=1) * sin

    def project(s):
        x = pair(acts, s)
        cos, sin = pair_rows(cos_ref, s), pair_rows(sin_ref, s)
        for start in range(0, n_q + 2, 2):
            width = min(2, n_q + 2 - start)
            res = jnp.dot(x, wqkv[:, start * head : (start + width) * head], preferred_element_type=F32)
            for i in range(width):
                h, states = start + i, res[:, i * head : (i + 1) * head]
                if h < n_q:
                    q_buf[s, h] = (rope(states, cos, sin) * QUERY_SCALE).astype(BF16)
                else:
                    val = (rope(states, cos, sin) if h == n_q else states).astype(BF16)
                    dst = k_buf if h == n_q else v_buf
                    dst[block_rows(mine(s)), :] = val[:rows]
                    dst[block_rows(theirs(s)), :] = val[rows:]

    for s in range(chips):
        if s < chips - 1:
            def body(j, _):
                ag_forward(acts, s + 1, j)
                return 0
        ag_join(acts, s)
        project(s)
        if s < chips - 1:
            lax.fori_loop(0, PIECES, body, 0)

    def attend(s):
        key_pos = prow_ref[...]
        offset = pair_rows(pcol_ref, s)[:, 0:1] - key_pos
        keep = (offset >= 0) & (offset < WINDOW)

        for h in range(n_q):
            scores = lax.dot_general(q_buf[s, h], k_buf[...], NT, preferred_element_type=F32)
            capped = SOFT_CAP * jnp.tanh(scores * (1.0 / SOFT_CAP))
            weight = jnp.where(keep, jnp.exp(capped), 0.0)
            total = jnp.sum(weight, axis=-1, keepdims=True)
            probs = (weight * (1.0 / total)).astype(BF16)
            mix = jnp.dot(probs, v_buf[...], preferred_element_type=F32)
            o_buf[:, h * head : (h + 1) * head] = mix.astype(BF16)

    def spread(s, lhs_ref, w_ref):
        @pl.loop(0, dim // SPREAD)
        def _(i):
            cols = pl.ds(pl.multiple_of(i * SPREAD, SPREAD), SPREAD)
            res = jnp.dot(lhs_ref[...], w_ref[:, cols], preferred_element_type=F32).astype(BF16)
            give[s, :, cols] = res[rows:]
            own[s, :, cols] = res[:rows]
        rs_chip_cols(s, 0).start()

    w_copies[n_qkv].wait()
    for i in range(chips):
        s = (i + 1) % chips
        attend(s)
        if i == 1:
            rs_stage(1, 0)
        spread(s, o_buf, wo)
    for t in range(1, chips - 1):
        rs_stage(1, t)
    ag_drain(acts)

    def att_finish(j, y):
        x1 = (e_own[sub(j), :].astype(F32) + norm_rows(y.astype(F32), g2_ref[...]).astype(F32)).astype(BF16)
        x_own[sub(j), :] = x1
        acts2[mine(0), sub(j), :] = norm_rows(x1.astype(F32), g3_ref[...])
        ag_begin(acts2, j)

    rs_last(1, att_finish)
    ring_drain(1)
    cols_drain()

    for copy in w_copies[n_qkv + 1 :]:
        copy.wait()
    n_tiles = ffn // FFN_TILE
    per_tile = PIECES // n_tiles

    def gate_up(s, i):
        x = pair(acts2, s)
        cols = pl.ds(i * FFN_TILE, FFN_TILE)
        gate = jnp.dot(x, wg[:, cols], preferred_element_type=F32)
        up = jnp.dot(x, wu[:, cols], preferred_element_type=F32)
        h_buf[:, cols] = (jax.nn.gelu(gate, approximate=True) * up).astype(BF16)

    for s in range(chips):
        ag_join(acts2, s)
        if s == chips - 2:
            rs_stage(2, 0)
        for i in range(n_tiles):
            gate_up(s, i)
            if s < chips - 1:
                for j in range(i * per_tile, (i + 1) * per_tile):
                    ag_forward(acts2, s + 1, j)
        spread(s, h_buf, wd)
    for t in range(1, chips - 1):
        rs_stage(2, t)
    ag_drain(acts2)

    def ffn_finish(j, z):
        out = x_own[sub(j), :].astype(F32) + norm_rows(z.astype(F32), g4_ref[...]).astype(F32)
        out_ref[sub(j), :] = out.astype(BF16)

    rs_last(2, ffn_finish)
    ring_drain(2)
    cols_drain()


def lookup_kernel(n_dev, tok_ref, tokrow_ref, table_hbm, out_ref, slots, tokcol, counts, sem):
    vocab, dim = table_hbm.shape
    seq_len = out_ref.shape[0]
    base = lax.axis_index("tp") * vocab
    n_blocks = seq_len // TOKENS
    unit = 8

    for g in range(n_blocks):
        def issue(i, count):
            for u in range(UNROLL):
                local = tok_ref[0, g * TOKENS + i * UNROLL + u] - base
                inside = (local >= 0) & (local < vocab)

                @pl.when(inside)
                def _():
                    src = pl.multiple_of(lax.shift_left(lax.shift_right_logical(local, 3), 3), unit)
                    dst = pl.multiple_of((g * TOKENS + count) * unit, unit)
                    pltpu.make_async_copy(table_hbm.at[pl.ds(src, unit), :], slots.at[pl.ds(dst, unit), :], sem.at[g]).start()
                count = count + jnp.where(inside, 1, 0)
            return count
        counts[g] = lax.fori_loop(0, TOKENS // UNROLL, issue, jnp.int32(0))

    tokcol[...] = jnp.transpose(jnp.broadcast_to(tokrow_ref[...], (TOKENS, seq_len)))
    scale = jnp.sqrt(jnp.float32(dim)).astype(BF16).astype(F32)
    depth = 256
    before = lax.broadcasted_iota(jnp.int32, (TOKENS, TOKENS), 1) < lax.broadcasted_iota(jnp.int32, (TOKENS, TOKENS), 0)
    col = lax.broadcasted_iota(jnp.int32, (TOKENS, depth), 1)
    slot_row = lax.broadcasted_iota(jnp.int32, (depth, dim), 0)

    for g in range(n_blocks):
        count = counts[g]

        def wait(i, _):
            pltpu.make_async_copy(table_hbm.at[pl.ds(0, unit), :], slots.at[pl.ds(0, unit), :], sem.at[g]).wait()
            return 0
        lax.fori_loop(0, count, wait, 0)
        span = slice(g * TOKENS, (g + 1) * TOKENS)
        row = tokrow_ref[:, span] - base
        row_in = ((row >= 0) & (row < vocab)).astype(F32)
        place = jnp.sum(jnp.where(before, row_in, 0.0), axis=1, keepdims=True).astype(jnp.int32)
        local = tokcol[span, 0:1] - base
        inside = (local >= 0) & (local < vocab)
        want = jnp.where(inside, place * unit + (local & 7), -1)

        def pick(kt):
            first = pl.multiple_of((g * TOKENS * unit) + kt * depth, depth)
            hot = (col + kt * depth == want).astype(F32).astype(BF16)
            held = jnp.where(slot_row + kt * depth < count * unit, slots[pl.ds(first, depth), :], jnp.zeros((), BF16))
            return (jnp.dot(hot, held, preferred_element_type=F32) * scale).astype(BF16)

        out_ref[span, :] = pick(0)

        def more(kt, _):
            out_ref[span, :] = out_ref[span, :] + pick(kt)
            return 0
        lax.fori_loop(1, lax.div(count * unit + depth - 1, depth), more, 0)


def lookup(n_dev, tokens, embed_block):
    seq_len, dim = tokens.shape[1], embed_block.shape[1]
    return pl.pallas_call(
        functools.partial(lookup_kernel, n_dev),
        name="lookup",
        out_shape=jax.ShapeDtypeStruct((seq_len, dim), BF16),
        in_specs=[pl.BlockSpec(memory_space=pltpu.SMEM), pl.BlockSpec(memory_space=pltpu.VMEM), pl.BlockSpec(memory_space=pl.ANY)],
        out_specs=pl.BlockSpec(memory_space=pltpu.VMEM),
        scratch_shapes=[
            pltpu.VMEM((8 * seq_len, dim), BF16),
            pltpu.VMEM((seq_len, TOKENS), jnp.int32),
            pltpu.SMEM((seq_len // TOKENS,), jnp.int32),
            pltpu.SemaphoreType.DMA((seq_len // TOKENS,)),
        ],
        compiler_params=pltpu.CompilerParams(vmem_limit_bytes=48 * 1024 * 1024),
    )(tokens, tokens, embed_block)


def decoder_layer(n_dev, part, positions, w_query, w_key, w_value, w_out, w_gate, w_up, w_down, g1, g2, g3, g4):
    seq_len = positions.shape[1]
    dim, n_q, head = w_query.shape
    ffn = w_gate.shape[1]
    chips, rows = n_dev // 2, seq_len // n_dev
    inv_freq = ROPE_BASE ** (-2.0 * jnp.arange(head // 2, dtype=F32) / head)
    freq = jnp.concatenate([inv_freq, inv_freq])[None, :]
    vmem = pl.BlockSpec(memory_space=pltpu.VMEM)
    hbm = pl.BlockSpec(memory_space=pltpu.HBM)
    block = (rows, dim)
    dma = pltpu.SemaphoreType.DMA
    weights = (
        w_query.transpose(1, 0, 2), w_key.reshape(dim, head), w_value.reshape(dim, head), w_out.reshape(n_q * head, dim),
        w_gate, w_up, w_down,
    )
    weights = [pltpu.with_memory_space_constraint(w, pltpu.HBM) for w in weights]
    return pl.pallas_call(
        functools.partial(layer_kernel, n_dev),
        name="layer",
        out_shape=jax.ShapeDtypeStruct((rows, dim), BF16),
        in_specs=[vmem] * 3 + [hbm] * 7 + [vmem] * 4,
        out_specs=vmem,
        scratch_shapes=[
            pltpu.VMEM((dim, (n_q + 2) * head), BF16),
            pltpu.VMEM((n_q * head, dim), BF16),
            pltpu.VMEM((dim, ffn), BF16),
            pltpu.VMEM((dim, ffn), BF16),
            pltpu.VMEM((ffn, dim), BF16),
            pltpu.VMEM((n_dev,) + block, BF16),
            pltpu.VMEM((n_dev,) + block, BF16),
            pltpu.VMEM((seq_len, head), F32),
            pltpu.VMEM((seq_len, head), F32),
            pltpu.VMEM((seq_len, head), jnp.int32),
            pltpu.VMEM((chips,) + block, BF16),
            pltpu.VMEM((chips,) + block, BF16),
            pltpu.VMEM((chips,) + block, BF16),
            pltpu.VMEM((chips - 1,) + block, BF16),
            pltpu.VMEM((2 * (chips - 1),) + block, BF16),
            pltpu.VMEM((chips, n_q, 2 * rows, head), BF16),
            pltpu.VMEM((seq_len, head), BF16),
            pltpu.VMEM((seq_len, head), BF16),
            pltpu.VMEM((2 * rows, n_q * head), BF16),
            pltpu.VMEM((2 * rows, ffn), BF16),
            pltpu.VMEM(block, BF16),
            pltpu.VMEM(block, BF16),
            dma((n_q + 6,)),
            dma((chips - 1, PIECES)),
            dma((chips - 1, PIECES)),
            dma((chips, 8)),
            dma((chips, 8)),
            dma((chips - 1, PIECES)),
            dma((2 * (chips - 1), PIECES)),
            dma((chips, 8)),
            dma((chips, 8)),
        ],
        compiler_params=pltpu.CompilerParams(collective_id=0, has_side_effects=True, vmem_limit_bytes=46 * 1024 * 1024),
    )(
        pltpu.with_memory_space_constraint(part.reshape((n_dev,) + block), pltpu.VMEM), freq, positions, *weights, g1.reshape(1, dim), g2.reshape(1, dim), g3.reshape(1, dim), g4.reshape(1, dim),
    )


def solution(mesh):
    n_dev = mesh.shape["tp"]
    in_specs = (P("dp", None), P("dp", None), P("tp", None), P(None, "tp", None), P(None, "tp", None), P(None, "tp", None), P("tp", None, None), P(None, "tp"), P(None, "tp"), P("tp", None), P(None), P(None), P(None), P(None))

    def device_step(tokens, positions, embed_block, *weights):
        part = lookup(n_dev, tokens, embed_block)
        return decoder_layer(n_dev, part, positions, *weights)[None]

    return jax.shard_map(device_step, mesh=mesh, in_specs=in_specs, out_specs=P("dp", "tp", None), check_vma=False)
```

```python
import functools

import jax
import jax.numpy as jnp
from jax import lax
from jax.experimental import pallas as pl
from jax.experimental.pallas import tpu as pltpu
from jax.sharding import PartitionSpec as P

WINDOW = 4096
QUERY_SCALE = 256.0 ** -0.5
SOFT_CAP = 50.0
NORM_EPS = 1e-6
ROPE_BASE = 10000.0
MESH = pl.DeviceIdType.MESH
BF16 = jnp.bfloat16
F32 = jnp.float32
PIECES = 4
FFN_TILE = 512
TOKENS = 128
NT = (((1,), (1,)), ((), ()))


def norm_rows(hidden, scale):
    mean_sq = jnp.mean(hidden * hidden, axis=-1, keepdims=True)
    return (hidden * lax.rsqrt(mean_sq + NORM_EPS) * (1.0 + scale)).astype(BF16)


def layer_kernel(
    n_dev, part, freq_ref, prow_ref, wq_hbm, wk_hbm, wv_hbm, wo_hbm, wg_hbm, wu_hbm, wd_hbm,
    g1_ref, g2_ref, g3_ref, g4_ref, out_ref,
    wqkv, wo, wg, wu, wd, acts, acts2, cos_ref, sin_ref, pcol_ref, own, give, take, ring_out, ring_in, q_buf, k_buf, v_buf, o_buf, h_buf, e_own, x_own,
    w_sem, ag_s, ag_r, agd_s, agd_r, rs_s, rs_r, rsd_s, rsd_r,
):
    chips = n_dev // 2
    rows = e_own.shape[0]
    piece = rows // PIECES
    dim = e_own.shape[1]
    n_q, head = q_buf.shape[1], q_buf.shape[3]
    ffn = h_buf.shape[1]

    me = lax.axis_index("tp")
    chip, core = lax.div(me, 2), lax.rem(me, 2)
    step = 1 - 2 * core
    partner = {"tp": me + step}
    ahead = {"tp": 2 * lax.rem(chip + step + chips, chips) + core}
    behind = {"tp": 2 * lax.rem(chip - step + chips, chips) + core}

    def mine(s):
        return 2 * lax.rem(chip - step * s + 2 * chips, chips) + core

    def theirs(s):
        return 2 * lax.rem(chip + step * s + 2 * chips, chips) + 1 - core

    def sub(j):
        return pl.ds(pl.multiple_of(j * piece, piece), piece)

    def block_rows(b):
        return pl.ds(pl.multiple_of(b * rows, rows), rows)

    w_copies = [pltpu.make_async_copy(wq_hbm.at[h], wqkv.at[:, pl.ds(h * head, head)], w_sem.at[h]) for h in range(n_q)]
    w_copies.append(pltpu.make_async_copy(wk_hbm, wqkv.at[:, pl.ds(n_q * head, head)], w_sem.at[n_q]))
    w_copies.append(pltpu.make_async_copy(wv_hbm, wqkv.at[:, pl.ds((n_q + 1) * head, head)], w_sem.at[n_q + 1]))
    n_qkv = len(w_copies)
    for i, (src, dst) in enumerate(((wo_hbm, wo), (wg_hbm, wg), (wu_hbm, wu), (wd_hbm, wd))):
        w_copies.append(pltpu.make_async_copy(src, dst, w_sem.at[n_qkv + i]))
    for copy in w_copies:
        copy.start()

    barrier = pltpu.get_barrier_semaphore()
    for peer in (partner, ahead, behind):
        pl.semaphore_signal(barrier, inc=1, device_id=peer, device_id_type=MESH)
    pl.semaphore_wait(barrier, 3)

    def remote(src, dst, send, recv, peer):
        return pltpu.make_async_remote_copy(
            src_ref=src, dst_ref=dst, send_sem=send, recv_sem=recv, device_id=peer, device_id_type=MESH
        )

    def ag_ring(buf, s, j, b):
        return remote(buf.at[b, sub(j)], buf.at[b, sub(j)], ag_s.at[s, j], ag_r.at[s, j], ahead)

    def ag_chip(buf, s, j, b):
        return remote(buf.at[b, sub(j)], buf.at[b, sub(j)], agd_s.at[s, j], agd_r.at[s, j], partner)

    def ag_begin(buf, j):
        ag_ring(buf, 0, j, mine(0)).start()
        ag_chip(buf, 0, j, mine(0)).start()

    def ag_forward(buf, s, j):
        ag_ring(buf, s - 1, j, mine(s)).wait_recv()
        if s < chips - 1:
            ag_ring(buf, s, j, mine(s)).start()
        ag_chip(buf, s, j, mine(s)).start()

    def ag_join(buf, s):
        def body(j, _):
            ag_chip(buf, s, j, theirs(s)).wait_recv()
            return 0
        lax.fori_loop(0, PIECES, body, 0)

    def ag_drain(buf):
        def body(j, _):
            for s in range(chips):
                if s < chips - 1:
                    ag_ring(buf, s, j, mine(s)).wait_send()
                ag_chip(buf, s, j, mine(s)).wait_send()
            return 0
        lax.fori_loop(0, PIECES, body, 0)

    def rs_chip_rows(s, j, b):
        return remote(part.at[b, sub(j)], take.at[s, sub(j)], rsd_s.at[s, j], rsd_r.at[s, j], partner)

    def rs_chip_block(s):
        return remote(give.at[s], take.at[s], rsd_s.at[s, 0], rsd_r.at[s, 0], partner)

    def rs_ring(r, t, j):
        slot = (r % 2) * (chips - 1) + t
        return remote(ring_out.at[t, sub(j)], ring_in.at[slot, sub(j)], rs_s.at[t, j], rs_r.at[slot, j], ahead)

    def rs_sum(r, t, j, own_ref):
        s = (t + 1) % chips
        total = own_ref[sub(j), :].astype(F32) + take[s, sub(j), :].astype(F32)
        if t > 0:
            rs_ring(r, t - 1, j).wait_recv()
            total = total + ring_in[(r % 2) * (chips - 1) + t - 1, sub(j), :].astype(F32)
        return total.astype(BF16)

    def rs_piece(r, t, own_ref, j):
        ring_out[t, sub(j), :] = rs_sum(r, t, j, own_ref)
        rs_ring(r, t, j).start()

    def rs_stage(r, t):
        rs_chip_block(t + 1).wait_recv()

        def body(j, _):
            rs_piece(r, t, own.at[t + 1], j)
            return 0
        lax.fori_loop(0, PIECES, body, 0)

    def rs_last(r, finish):
        rs_chip_block(0).wait_recv()

        def body(j, _):
            finish(j, rs_sum(r, chips - 1, j, own.at[0]))
            return 0
        lax.fori_loop(0, PIECES, body, 0)

    def ring_drain(r):
        def body(j, _):
            for t in range(chips - 1):
                rs_ring(r, t, j).wait_send()
            return 0
        lax.fori_loop(0, PIECES, body, 0)

    def block_drain():
        for s in range(chips):
            rs_chip_block(s).wait_send()

    seq_len = prow_ref.shape[1]
    table_rows = seq_len // ((chips - 2) * PIECES)
    pcol_ref[...] = jnp.transpose(jnp.broadcast_to(prow_ref[...], (head, seq_len)))

    def rotary(i):
        span = pl.ds(pl.multiple_of(i * table_rows, table_rows), table_rows)
        angles = pcol_ref[span, :].astype(F32) * freq_ref[...]
        lane = lax.broadcasted_iota(jnp.int32, angles.shape, 1)
        cos_ref[span, :] = jnp.cos(angles)
        sin = jnp.sin(angles)
        sin_ref[span, :] = jnp.where(lane < head // 2, -sin, sin)

    for s in range(chips):
        def body(j, _):
            rs_chip_rows((s + 1) % chips, j, theirs(s + 1)).start()
            return 0
        lax.fori_loop(0, PIECES, body, 0)
    for t in range(chips - 1):
        def body(j, _):
            rs_chip_rows(t + 1, j, theirs(t + 1)).wait_recv()
            rs_piece(0, t, part.at[mine(t + 1)], j)
            if t < chips - 2:
                rotary(t * PIECES + j)
            return 0
        lax.fori_loop(0, PIECES, body, 0)

    def emb_finish(j, _):
        rs_chip_rows(0, j, theirs(0)).wait_recv()
        e = rs_sum(0, chips - 1, j, part.at[mine(0)])
        e_own[sub(j), :] = e
        acts[mine(0), sub(j), :] = norm_rows(e.astype(F32), g1_ref[...])
        ag_begin(acts, j)
        return 0
    lax.fori_loop(0, PIECES, emb_finish, 0)
    ring_drain(0)

    def emb_drain(j, _):
        for s in range(chips):
            rs_chip_rows(s, j, theirs(s)).wait_send()
        return 0
    lax.fori_loop(0, PIECES, emb_drain, 0)

    for copy in w_copies[:n_qkv]:
        copy.wait()

    def pair(ref, s):
        return jnp.concatenate([ref[mine(s)], ref[theirs(s)]], axis=0)

    def pair_rows(ref, s):
        return jnp.concatenate([ref[block_rows(mine(s)), :], ref[block_rows(theirs(s)), :]], axis=0)

    def rope(states, cos, sin):
        return states * cos + pltpu.roll(states, head // 2, axis=1) * sin

    def project(s):
        x = pair(acts, s)
        cos, sin = pair_rows(cos_ref, s), pair_rows(sin_ref, s)
        for start in range(0, n_q + 2, 2):
            width = min(2, n_q + 2 - start)
            res = jnp.dot(x, wqkv[:, start * head : (start + width) * head], preferred_element_type=F32)
            for i in range(width):
                h, states = start + i, res[:, i * head : (i + 1) * head]
                if h < n_q:
                    q_buf[s, h] = (rope(states, cos, sin) * QUERY_SCALE).astype(BF16)
                else:
                    val = (rope(states, cos, sin) if h == n_q else states).astype(BF16)
                    dst = k_buf if h == n_q else v_buf
                    dst[block_rows(mine(s)), :] = val[:rows]
                    dst[block_rows(theirs(s)), :] = val[rows:]

    for s in range(chips):
        if s < chips - 1:
            def body(j, _):
                ag_forward(acts, s + 1, j)
                return 0
        ag_join(acts, s)
        project(s)
        if s < chips - 1:
            lax.fori_loop(0, PIECES, body, 0)

    def attend(s):
        key_pos = prow_ref[...]
        offset = pair_rows(pcol_ref, s)[:, 0:1] - key_pos
        keep = (offset >= 0) & (offset < WINDOW)

        for h in range(n_q):
            scores = lax.dot_general(q_buf[s, h], k_buf[...], NT, preferred_element_type=F32)
            capped = SOFT_CAP * jnp.tanh(scores * (1.0 / SOFT_CAP))
            weight = jnp.where(keep, jnp.exp(capped), 0.0)
            total = jnp.sum(weight, axis=-1, keepdims=True)
            probs = (weight * (1.0 / total)).astype(BF16)
            mix = jnp.dot(probs, v_buf[...], preferred_element_type=F32)
            o_buf[:, h * head : (h + 1) * head] = mix.astype(BF16)

    def spread(s, lhs_ref, w_ref):
        res = jnp.dot(lhs_ref[...], w_ref[...], preferred_element_type=F32).astype(BF16)
        give[s] = res[rows:]
        own[s] = res[:rows]
        rs_chip_block(s).start()

    w_copies[n_qkv].wait()
    for i in range(chips):
        s = (i + 1) % chips
        attend(s)
        if i == 1:
            rs_stage(1, 0)
        spread(s, o_buf, wo)
    for t in range(1, chips - 1):
        rs_stage(1, t)
    ag_drain(acts)

    def att_finish(j, y):
        x1 = (e_own[sub(j), :].astype(F32) + norm_rows(y.astype(F32), g2_ref[...]).astype(F32)).astype(BF16)
        x_own[sub(j), :] = x1
        acts2[mine(0), sub(j), :] = norm_rows(x1.astype(F32), g3_ref[...])
        ag_begin(acts2, j)

    rs_last(1, att_finish)
    ring_drain(1)
    block_drain()

    for copy in w_copies[n_qkv + 1 :]:
        copy.wait()
    n_tiles = ffn // FFN_TILE
    per_tile = PIECES // n_tiles

    def gate_up(s, i):
        x = pair(acts2, s)
        cols = pl.ds(i * FFN_TILE, FFN_TILE)
        gate = jnp.dot(x, wg[:, cols], preferred_element_type=F32)
        up = jnp.dot(x, wu[:, cols], preferred_element_type=F32)
        h_buf[:, cols] = (jax.nn.gelu(gate, approximate=True) * up).astype(BF16)

    for s in range(chips):
        ag_join(acts2, s)
        if s == chips - 2:
            rs_stage(2, 0)
        if s == chips - 1:
            rs_chip_block(chips - 2).wait_recv()
        for i in range(n_tiles):
            gate_up(s, i)
            for j in range(i * per_tile, (i + 1) * per_tile):
                if s < chips - 1:
                    ag_forward(acts2, s + 1, j)
                else:
                    rs_piece(2, chips - 3, own.at[chips - 2], j)
        spread(s, h_buf, wd)
    rs_stage(2, chips - 2)
    ag_drain(acts2)

    def ffn_finish(j, z):
        out = x_own[sub(j), :].astype(F32) + norm_rows(z.astype(F32), g4_ref[...]).astype(F32)
        out_ref[sub(j), :] = out.astype(BF16)

    rs_last(2, ffn_finish)
    ring_drain(2)
    block_drain()


def lookup_kernel(tokrow_ref, table_hbm, out_ref, slots, tokcol, list_v, list_s, list_sem, sem):
    vocab, dim = table_hbm.shape
    seq_len = out_ref.shape[0]
    base = lax.axis_index("tp") * vocab
    n_blocks = seq_len // TOKENS
    unit = 8
    depth = 512
    square = (TOKENS, TOKENS)
    lane, line = lax.broadcasted_iota(jnp.int32, square, 1), lax.broadcasted_iota(jnp.int32, square, 0)
    tokcol[...] = jnp.transpose(jnp.broadcast_to(tokrow_ref[...], (TOKENS, seq_len)))

    wants = []
    for g in range(n_blocks):
        span = slice(g * TOKENS, (g + 1) * TOKENS)
        row = tokrow_ref[:, span] - base
        row_in = ((row >= 0) & (row < vocab)).astype(F32)
        place = jnp.sum(jnp.where(lane < line, row_in, 0.0), axis=1, keepdims=True).astype(jnp.int32)
        local = tokcol[span, 0:1] - base
        inside = (local >= 0) & (local < vocab)
        wants.append(jnp.where(inside, place * unit + (local & 7), -1))
        hits = jnp.where((lane == place) & inside, local.astype(F32), 0.0)
        list_v[g : g + 1, :] = jnp.sum(hits, axis=0, keepdims=True).astype(jnp.int32)
        total = jnp.sum(row_in, axis=1, keepdims=True).astype(jnp.int32)
        list_v[n_blocks + g : n_blocks + g + 1, :] = jnp.broadcast_to(total, (1, TOKENS))
    to_scalars = pltpu.make_async_copy(list_v, list_s, list_sem)
    to_scalars.start()
    to_scalars.wait()

    for g in range(n_blocks):
        def issue(i, _):
            local = list_s[g, i]
            src = pl.multiple_of(lax.shift_left(lax.shift_right_logical(local, 3), 3), unit)
            dst = pl.multiple_of((g * TOKENS + i) * unit, unit)
            pltpu.make_async_copy(table_hbm.at[pl.ds(src, unit), :], slots.at[pl.ds(dst, unit), :], sem.at[g]).start()
            return 0
        lax.fori_loop(0, list_s[n_blocks + g, 0], issue, 0)

    scale = jnp.sqrt(jnp.float32(dim)).astype(BF16).astype(F32)
    col = lax.broadcasted_iota(jnp.int32, (TOKENS, depth), 1)
    slot_row = lax.broadcasted_iota(jnp.int32, (depth, dim), 0)

    for g in range(n_blocks):
        count = list_s[n_blocks + g, 0]
        want = wants[g]

        def wait(i, _):
            pltpu.make_async_copy(table_hbm.at[pl.ds(0, unit), :], slots.at[pl.ds(0, unit), :], sem.at[g]).wait()
            return 0
        lax.fori_loop(0, count, wait, 0)
        span = slice(g * TOKENS, (g + 1) * TOKENS)

        def pick(kt):
            first = pl.multiple_of((g * TOKENS * unit) + kt * depth, depth)
            hot = (col + kt * depth == want).astype(F32).astype(BF16)
            held = jnp.where(slot_row + kt * depth < count * unit, slots[pl.ds(first, depth), :], jnp.zeros((), BF16))
            return (jnp.dot(hot, held, preferred_element_type=F32) * scale).astype(BF16)

        out_ref[span, :] = pick(0)

        def more(kt, _):
            out_ref[span, :] = out_ref[span, :] + pick(kt)
            return 0
        lax.fori_loop(1, lax.div(count * unit + depth - 1, depth), more, 0)


def lookup(tokens, embed_block):
    seq_len, dim = tokens.shape[1], embed_block.shape[1]
    return pl.pallas_call(
        lookup_kernel,
        name="lookup",
        out_shape=jax.ShapeDtypeStruct((seq_len, dim), BF16),
        in_specs=[pl.BlockSpec(memory_space=pltpu.VMEM), pl.BlockSpec(memory_space=pl.ANY)],
        out_specs=pl.BlockSpec(memory_space=pltpu.VMEM),
        scratch_shapes=[
            pltpu.VMEM((8 * seq_len, dim), BF16),
            pltpu.VMEM((seq_len, TOKENS), jnp.int32),
            pltpu.VMEM((2 * seq_len // TOKENS, TOKENS), jnp.int32),
            pltpu.SMEM((2 * seq_len // TOKENS, TOKENS), jnp.int32),
            pltpu.SemaphoreType.DMA,
            pltpu.SemaphoreType.DMA((seq_len // TOKENS,)),
        ],
        compiler_params=pltpu.CompilerParams(vmem_limit_bytes=48 * 1024 * 1024),
    )(tokens, embed_block)


def decoder_layer(n_dev, part, positions, w_query, w_key, w_value, w_out, w_gate, w_up, w_down, g1, g2, g3, g4):
    seq_len = positions.shape[1]
    dim, n_q, head = w_query.shape
    ffn = w_gate.shape[1]
    chips, rows = n_dev // 2, seq_len // n_dev
    inv_freq = ROPE_BASE ** (-2.0 * jnp.arange(head // 2, dtype=F32) / head)
    freq = jnp.concatenate([inv_freq, inv_freq])[None, :]
    vmem = pl.BlockSpec(memory_space=pltpu.VMEM)
    hbm = pl.BlockSpec(memory_space=pltpu.HBM)
    block = (rows, dim)
    dma = pltpu.SemaphoreType.DMA
    weights = (
        w_query.transpose(1, 0, 2), w_key.reshape(dim, head), w_value.reshape(dim, head), w_out.reshape(n_q * head, dim),
        w_gate, w_up, w_down,
    )
    weights = [pltpu.with_memory_space_constraint(w, pltpu.HBM) for w in weights]
    return pl.pallas_call(
        functools.partial(layer_kernel, n_dev),
        name="layer",
        out_shape=jax.ShapeDtypeStruct((rows, dim), BF16),
        in_specs=[vmem] * 3 + [hbm] * 7 + [vmem] * 4,
        out_specs=vmem,
        scratch_shapes=[
            pltpu.VMEM((dim, (n_q + 2) * head), BF16),
            pltpu.VMEM((n_q * head, dim), BF16),
            pltpu.VMEM((dim, ffn), BF16),
            pltpu.VMEM((dim, ffn), BF16),
            pltpu.VMEM((ffn, dim), BF16),
            pltpu.VMEM((n_dev,) + block, BF16),
            pltpu.VMEM((n_dev,) + block, BF16),
            pltpu.VMEM((seq_len, head), F32),
            pltpu.VMEM((seq_len, head), F32),
            pltpu.VMEM((seq_len, head), jnp.int32),
            pltpu.VMEM((chips,) + block, BF16),
            pltpu.VMEM((chips,) + block, BF16),
            pltpu.VMEM((chips,) + block, BF16),
            pltpu.VMEM((chips - 1,) + block, BF16),
            pltpu.VMEM((2 * (chips - 1),) + block, BF16),
            pltpu.VMEM((chips, n_q, 2 * rows, head), BF16),
            pltpu.VMEM((seq_len, head), BF16),
            pltpu.VMEM((seq_len, head), BF16),
            pltpu.VMEM((2 * rows, n_q * head), BF16),
            pltpu.VMEM((2 * rows, ffn), BF16),
            pltpu.VMEM(block, BF16),
            pltpu.VMEM(block, BF16),
            dma((n_q + 6,)),
            dma((chips - 1, PIECES)),
            dma((chips - 1, PIECES)),
            dma((chips, PIECES)),
            dma((chips, PIECES)),
            dma((chips - 1, PIECES)),
            dma((2 * (chips - 1), PIECES)),
            dma((chips, PIECES)),
            dma((chips, PIECES)),
        ],
        compiler_params=pltpu.CompilerParams(collective_id=0, has_side_effects=True, vmem_limit_bytes=46 * 1024 * 1024),
    )(
        pltpu.with_memory_space_constraint(part.reshape((n_dev,) + block), pltpu.VMEM), freq, positions, *weights, g1.reshape(1, dim), g2.reshape(1, dim), g3.reshape(1, dim), g4.reshape(1, dim),
    )


def solution(mesh):
    n_dev = mesh.shape["tp"]
    in_specs = (P("dp", None), P("dp", None), P("tp", None), P(None, "tp", None), P(None, "tp", None), P(None, "tp", None), P("tp", None, None), P(None, "tp"), P(None, "tp"), P("tp", None), P(None), P(None), P(None), P(None))

    def device_step(tokens, positions, embed_block, *weights):
        part = lookup(tokens, embed_block)
        return decoder_layer(n_dev, part, positions, *weights)[None]

    return jax.shard_map(device_step, mesh=mesh, in_specs=in_specs, out_specs=P("dp", "tp", None), check_vma=False)
```

```python
import functools

import jax
import jax.numpy as jnp
from jax import lax
from jax.experimental import pallas as pl
from jax.experimental.pallas import tpu as pltpu
from jax.sharding import PartitionSpec as P

WINDOW = 4096
QUERY_SCALE = 256.0 ** -0.5
SOFT_CAP = 50.0
NORM_EPS = 1e-6
ROPE_BASE = 10000.0
MESH = pl.DeviceIdType.MESH
BF16 = jnp.bfloat16
F32 = jnp.float32
PIECES = 4
FFN_TILE = 512
TOKENS = 128
NT = (((1,), (1,)), ((), ()))


def norm_rows(hidden, scale):
    mean_sq = jnp.mean(hidden * hidden, axis=-1, keepdims=True)
    return (hidden * lax.rsqrt(mean_sq + NORM_EPS) * (1.0 + scale)).astype(BF16)


def layer_kernel(
    n_dev, part, freq_ref, prow_ref, wq_hbm, wk_hbm, wv_hbm, wo_hbm, wg_hbm, wu_hbm, wd_hbm,
    g1_ref, g2_ref, g3_ref, g4_ref, out_ref,
    wqkv, wo, wg, wu, wd, acts, acts2, cos_ref, sin_ref, pcol_ref, own, give, take, ring_out, ring_in, q_buf, k_buf, v_buf, o_buf, h_buf, e_own, x_own,
    w_sem, ag_s, ag_r, agd_s, agd_r, rs_s, rs_r, rsd_s, rsd_r,
):
    chips = n_dev // 2
    rows = e_own.shape[0]
    piece = rows // PIECES
    dim = e_own.shape[1]
    n_q, head = q_buf.shape[1], q_buf.shape[3]
    ffn = h_buf.shape[1]

    me = lax.axis_index("tp")
    chip, core = lax.div(me, 2), lax.rem(me, 2)
    step = 1 - 2 * core
    partner = {"tp": me + step}
    ahead = {"tp": 2 * lax.rem(chip + step + chips, chips) + core}
    behind = {"tp": 2 * lax.rem(chip - step + chips, chips) + core}

    def mine(s):
        return 2 * lax.rem(chip - step * s + 2 * chips, chips) + core

    def theirs(s):
        return 2 * lax.rem(chip + step * s + 2 * chips, chips) + 1 - core

    def sub(j):
        return pl.ds(pl.multiple_of(j * piece, piece), piece)

    def block_rows(b):
        return pl.ds(pl.multiple_of(b * rows, rows), rows)

    w_copies = [pltpu.make_async_copy(wq_hbm.at[h], wqkv.at[:, pl.ds(h * head, head)], w_sem.at[h]) for h in range(n_q)]
    w_copies.append(pltpu.make_async_copy(wk_hbm, wqkv.at[:, pl.ds(n_q * head, head)], w_sem.at[n_q]))
    w_copies.append(pltpu.make_async_copy(wv_hbm, wqkv.at[:, pl.ds((n_q + 1) * head, head)], w_sem.at[n_q + 1]))
    n_qkv = len(w_copies)
    for i, (src, dst) in enumerate(((wo_hbm, wo), (wg_hbm, wg), (wu_hbm, wu), (wd_hbm, wd))):
        w_copies.append(pltpu.make_async_copy(src, dst, w_sem.at[n_qkv + i]))
    for copy in w_copies:
        copy.start()

    barrier = pltpu.get_barrier_semaphore()
    for peer in (partner, ahead, behind):
        pl.semaphore_signal(barrier, inc=1, device_id=peer, device_id_type=MESH)
    pl.semaphore_wait(barrier, 3)

    def remote(src, dst, send, recv, peer):
        return pltpu.make_async_remote_copy(
            src_ref=src, dst_ref=dst, send_sem=send, recv_sem=recv, device_id=peer, device_id_type=MESH
        )

    def ag_ring(buf, s, j, b):
        return remote(buf.at[b, sub(j)], buf.at[b, sub(j)], ag_s.at[s, j], ag_r.at[s, j], ahead)

    def ag_chip(buf, s, j, b):
        return remote(buf.at[b, sub(j)], buf.at[b, sub(j)], agd_s.at[s, j], agd_r.at[s, j], partner)

    def ag_begin(buf, j):
        ag_ring(buf, 0, j, mine(0)).start()
        ag_chip(buf, 0, j, mine(0)).start()

    def ag_forward(buf, s, j):
        ag_ring(buf, s - 1, j, mine(s)).wait_recv()
        if s < chips - 1:
            ag_ring(buf, s, j, mine(s)).start()
        ag_chip(buf, s, j, mine(s)).start()

    def ag_join(buf, s):
        def body(j, _):
            ag_chip(buf, s, j, theirs(s)).wait_recv()
            return 0
        lax.fori_loop(0, PIECES, body, 0)

    def ag_drain(buf):
        def body(j, _):
            for s in range(chips):
                if s < chips - 1:
                    ag_ring(buf, s, j, mine(s)).wait_send()
                ag_chip(buf, s, j, mine(s)).wait_send()
            return 0
        lax.fori_loop(0, PIECES, body, 0)

    def rs_chip_rows(s, j, b):
        return remote(part.at[b, sub(j)], take.at[s, sub(j)], rsd_s.at[s, j], rsd_r.at[s, j], partner)

    def rs_chip_give(s, j):
        return remote(give.at[s, sub(j)], take.at[s, sub(j)], rsd_s.at[s, j], rsd_r.at[s, j], partner)

    def rs_ring(r, t, j):
        slot = (r % 2) * (chips - 1) + t
        return remote(ring_out.at[t, sub(j)], ring_in.at[slot, sub(j)], rs_s.at[t, j], rs_r.at[slot, j], ahead)

    def rs_sum(r, t, j, own_ref):
        s = (t + 1) % chips
        total = own_ref[sub(j), :].astype(F32) + take[s, sub(j), :].astype(F32)
        if t > 0:
            rs_ring(r, t - 1, j).wait_recv()
            total = total + ring_in[(r % 2) * (chips - 1) + t - 1, sub(j), :].astype(F32)
        return total.astype(BF16)

    def rs_piece(r, t, own_ref, j):
        ring_out[t, sub(j), :] = rs_sum(r, t, j, own_ref)
        rs_ring(r, t, j).start()

    def rs_stage(r, t):
        def body(j, _):
            rs_chip_give(t + 1, j).wait_recv()
            rs_piece(r, t, own.at[t + 1], j)
            return 0
        lax.fori_loop(0, PIECES, body, 0)

    def rs_last(r, finish):
        def body(j, _):
            rs_chip_give(0, j).wait_recv()
            finish(j, rs_sum(r, chips - 1, j, own.at[0]))
            return 0
        lax.fori_loop(0, PIECES, body, 0)

    def ring_drain(r):
        def body(j, _):
            for t in range(chips - 1):
                rs_ring(r, t, j).wait_send()
            return 0
        lax.fori_loop(0, PIECES, body, 0)

    def block_drain():
        def body(j, _):
            for s in range(chips):
                rs_chip_give(s, j).wait_send()
            return 0
        lax.fori_loop(0, PIECES, body, 0)

    seq_len = prow_ref.shape[1]
    table_rows = seq_len // ((chips - 2) * PIECES)
    pcol_ref[...] = jnp.transpose(jnp.broadcast_to(prow_ref[...], (head, seq_len)))

    def rotary(i):
        span = pl.ds(pl.multiple_of(i * table_rows, table_rows), table_rows)
        angles = pcol_ref[span, :].astype(F32) * freq_ref[...]
        lane = lax.broadcasted_iota(jnp.int32, angles.shape, 1)
        cos_ref[span, :] = jnp.cos(angles)
        sin = jnp.sin(angles)
        sin_ref[span, :] = jnp.where(lane < head // 2, -sin, sin)

    for s in range(chips):
        def body(j, _):
            rs_chip_rows((s + 1) % chips, j, theirs(s + 1)).start()
            return 0
        lax.fori_loop(0, PIECES, body, 0)
    for t in range(chips - 1):
        def body(j, _):
            rs_chip_rows(t + 1, j, theirs(t + 1)).wait_recv()
            rs_piece(0, t, part.at[mine(t + 1)], j)
            if t < chips - 2:
                rotary(t * PIECES + j)
            return 0
        lax.fori_loop(0, PIECES, body, 0)

    def emb_finish(j, _):
        rs_chip_rows(0, j, theirs(0)).wait_recv()
        e = rs_sum(0, chips - 1, j, part.at[mine(0)])
        e_own[sub(j), :] = e
        acts[mine(0), sub(j), :] = norm_rows(e.astype(F32), g1_ref[...])
        ag_begin(acts, j)
        return 0
    lax.fori_loop(0, PIECES, emb_finish, 0)
    ring_drain(0)

    def emb_drain(j, _):
        for s in range(chips):
            rs_chip_rows(s, j, theirs(s)).wait_send()
        return 0
    lax.fori_loop(0, PIECES, emb_drain, 0)

    for copy in w_copies[:n_qkv]:
        copy.wait()

    def pair(ref, s):
        return jnp.concatenate([ref[mine(s)], ref[theirs(s)]], axis=0)

    def pair_rows(ref, s):
        return jnp.concatenate([ref[block_rows(mine(s)), :], ref[block_rows(theirs(s)), :]], axis=0)

    def rope(states, cos, sin):
        return states * cos + pltpu.roll(states, head // 2, axis=1) * sin

    def project(s):
        x = pair(acts, s)
        cos, sin = pair_rows(cos_ref, s), pair_rows(sin_ref, s)
        for start in range(0, n_q + 2, 2):
            width = min(2, n_q + 2 - start)
            res = jnp.dot(x, wqkv[:, start * head : (start + width) * head], preferred_element_type=F32)
            for i in range(width):
                h, states = start + i, res[:, i * head : (i + 1) * head]
                if h < n_q:
                    q_buf[s, h] = (rope(states, cos, sin) * QUERY_SCALE).astype(BF16)
                else:
                    val = (rope(states, cos, sin) if h == n_q else states).astype(BF16)
                    dst = k_buf if h == n_q else v_buf
                    dst[block_rows(mine(s)), :] = val[:rows]
                    dst[block_rows(theirs(s)), :] = val[rows:]

    for s in range(chips):
        if s < chips - 1:
            def body(j, _):
                ag_forward(acts, s + 1, j)
                return 0
        ag_join(acts, s)
        project(s)
        if s < chips - 1:
            lax.fori_loop(0, PIECES, body, 0)

    def attend(s):
        key_pos = prow_ref[...]
        offset = pair_rows(pcol_ref, s)[:, 0:1] - key_pos
        keep = (offset >= 0) & (offset < WINDOW)

        for h in range(n_q):
            scores = lax.dot_general(q_buf[s, h], k_buf[...], NT, preferred_element_type=F32)
            capped = SOFT_CAP * jnp.tanh(scores * (1.0 / SOFT_CAP))
            weight = jnp.where(keep, jnp.exp(capped), 0.0)
            total = jnp.sum(weight, axis=-1, keepdims=True)
            probs = (weight * (1.0 / total)).astype(BF16)
            mix = jnp.dot(probs, v_buf[...], preferred_element_type=F32)
            o_buf[:, h * head : (h + 1) * head] = mix.astype(BF16)

    def spread(s, lhs_ref, w_ref):
        res = jnp.dot(lhs_ref[...], w_ref[...], preferred_element_type=F32).astype(BF16)
        give[s] = res[rows:]
        own[s] = res[:rows]
        for j in range(PIECES):
            rs_chip_give(s, j).start()

    w_copies[n_qkv].wait()
    for i in range(chips):
        s = (i + 1) % chips
        attend(s)
        if i == 1:
            rs_stage(1, 0)
        spread(s, o_buf, wo)
    for t in range(1, chips - 1):
        rs_stage(1, t)
    ag_drain(acts)

    def att_finish(j, y):
        x1 = (e_own[sub(j), :].astype(F32) + norm_rows(y.astype(F32), g2_ref[...]).astype(F32)).astype(BF16)
        x_own[sub(j), :] = x1
        acts2[mine(0), sub(j), :] = norm_rows(x1.astype(F32), g3_ref[...])
        ag_begin(acts2, j)

    rs_last(1, att_finish)
    ring_drain(1)
    block_drain()

    for copy in w_copies[n_qkv + 1 :]:
        copy.wait()
    n_tiles = ffn // FFN_TILE
    per_tile = PIECES // n_tiles

    def gate_up(s, i):
        x = pair(acts2, s)
        cols = pl.ds(i * FFN_TILE, FFN_TILE)
        gate = jnp.dot(x, wg[:, cols], preferred_element_type=F32)
        up = jnp.dot(x, wu[:, cols], preferred_element_type=F32)
        h_buf[:, cols] = (jax.nn.gelu(gate, approximate=True) * up).astype(BF16)

    for s in range(chips):
        ag_join(acts2, s)
        if s == chips - 2:
            rs_stage(2, 0)
        for i in range(n_tiles):
            gate_up(s, i)
            for j in range(i * per_tile, (i + 1) * per_tile):
                if s < chips - 1:
                    ag_forward(acts2, s + 1, j)
                else:
                    rs_chip_give(chips - 2, j).wait_recv()
                    rs_piece(2, chips - 3, own.at[chips - 2], j)
        spread(s, h_buf, wd)
    rs_stage(2, chips - 2)
    ag_drain(acts2)

    def ffn_finish(j, z):
        out = x_own[sub(j), :].astype(F32) + norm_rows(z.astype(F32), g4_ref[...]).astype(F32)
        out_ref[sub(j), :] = out.astype(BF16)

    rs_last(2, ffn_finish)
    ring_drain(2)
    block_drain()


def lookup_kernel(tokrow_ref, table_hbm, out_ref, slots, tokcol, list_v, list_s, list_sem, sem):
    vocab, dim = table_hbm.shape
    seq_len = out_ref.shape[0]
    base = lax.axis_index("tp") * vocab
    n_blocks = seq_len // TOKENS
    unit = 8
    depth = 512
    square = (TOKENS, TOKENS)
    lane, line = lax.broadcasted_iota(jnp.int32, square, 1), lax.broadcasted_iota(jnp.int32, square, 0)
    tokcol[...] = jnp.transpose(jnp.broadcast_to(tokrow_ref[...], (TOKENS, seq_len)))

    wants = []
    for g in range(n_blocks):
        span = slice(g * TOKENS, (g + 1) * TOKENS)
        row = tokrow_ref[:, span] - base
        row_in = ((row >= 0) & (row < vocab)).astype(F32)
        place = jnp.sum(jnp.where(lane < line, row_in, 0.0), axis=1, keepdims=True).astype(jnp.int32)
        local = tokcol[span, 0:1] - base
        inside = (local >= 0) & (local < vocab)
        wants.append(jnp.where(inside, place * unit + (local & 7), -1))
        hits = jnp.where((lane == place) & inside, local.astype(F32), 0.0)
        list_v[g, 0:1, :] = jnp.sum(hits, axis=0, keepdims=True).astype(jnp.int32)
        total = jnp.sum(row_in, axis=1, keepdims=True).astype(jnp.int32)
        list_v[g, 1:2, :] = jnp.broadcast_to(total, (1, TOKENS))
        pltpu.make_async_copy(list_v.at[g], list_s.at[g], list_sem.at[g]).start()

    for g in range(n_blocks):
        pltpu.make_async_copy(list_v.at[g], list_s.at[g], list_sem.at[g]).wait()

        def issue(i, _):
            local = list_s[g, 0, i]
            src = pl.multiple_of(lax.shift_left(lax.shift_right_logical(local, 3), 3), unit)
            dst = pl.multiple_of((g * TOKENS + i) * unit, unit)
            pltpu.make_async_copy(table_hbm.at[pl.ds(src, unit), :], slots.at[pl.ds(dst, unit), :], sem.at[g]).start()
            return 0
        lax.fori_loop(0, list_s[g, 1, 0], issue, 0)

    scale = jnp.sqrt(jnp.float32(dim)).astype(BF16).astype(F32)
    col = lax.broadcasted_iota(jnp.int32, (TOKENS, depth), 1)
    slot_row = lax.broadcasted_iota(jnp.int32, (depth, dim), 0)

    for g in range(n_blocks):
        count = list_s[g, 1, 0]
        want = wants[g]

        def wait(i, _):
            pltpu.make_async_copy(table_hbm.at[pl.ds(0, unit), :], slots.at[pl.ds(0, unit), :], sem.at[g]).wait()
            return 0
        lax.fori_loop(0, count, wait, 0)
        span = slice(g * TOKENS, (g + 1) * TOKENS)

        def pick(kt):
            first = pl.multiple_of((g * TOKENS * unit) + kt * depth, depth)
            hot = (col + kt * depth == want).astype(F32).astype(BF16)
            held = jnp.where(slot_row + kt * depth < count * unit, slots[pl.ds(first, depth), :], jnp.zeros((), BF16))
            return (jnp.dot(hot, held, preferred_element_type=F32) * scale).astype(BF16)

        out_ref[span, :] = pick(0)

        def more(kt, _):
            out_ref[span, :] = out_ref[span, :] + pick(kt)
            return 0
        lax.fori_loop(1, lax.div(count * unit + depth - 1, depth), more, 0)


def lookup(tokens, embed_block):
    seq_len, dim = tokens.shape[1], embed_block.shape[1]
    return pl.pallas_call(
        lookup_kernel,
        name="lookup",
        out_shape=jax.ShapeDtypeStruct((seq_len, dim), BF16),
        in_specs=[pl.BlockSpec(memory_space=pltpu.VMEM), pl.BlockSpec(memory_space=pl.ANY)],
        out_specs=pl.BlockSpec(memory_space=pltpu.VMEM),
        scratch_shapes=[
            pltpu.VMEM((8 * seq_len, dim), BF16),
            pltpu.VMEM((seq_len, TOKENS), jnp.int32),
            pltpu.VMEM((seq_len // TOKENS, 8, TOKENS), jnp.int32),
            pltpu.SMEM((seq_len // TOKENS, 8, TOKENS), jnp.int32),
            pltpu.SemaphoreType.DMA((seq_len // TOKENS,)),
            pltpu.SemaphoreType.DMA((seq_len // TOKENS,)),
        ],
        compiler_params=pltpu.CompilerParams(vmem_limit_bytes=48 * 1024 * 1024),
    )(tokens, embed_block)


def decoder_layer(n_dev, part, positions, w_query, w_key, w_value, w_out, w_gate, w_up, w_down, g1, g2, g3, g4):
    seq_len = positions.shape[1]
    dim, n_q, head = w_query.shape
    ffn = w_gate.shape[1]
    chips, rows = n_dev // 2, seq_len // n_dev
    inv_freq = ROPE_BASE ** (-2.0 * jnp.arange(head // 2, dtype=F32) / head)
    freq = jnp.concatenate([inv_freq, inv_freq])[None, :]
    vmem = pl.BlockSpec(memory_space=pltpu.VMEM)
    hbm = pl.BlockSpec(memory_space=pltpu.HBM)
    block = (rows, dim)
    dma = pltpu.SemaphoreType.DMA
    weights = (
        w_query.transpose(1, 0, 2), w_key.reshape(dim, head), w_value.reshape(dim, head), w_out.reshape(n_q * head, dim),
        w_gate, w_up, w_down,
    )
    weights = [pltpu.with_memory_space_constraint(w, pltpu.HBM) for w in weights]
    return pl.pallas_call(
        functools.partial(layer_kernel, n_dev),
        name="layer",
        out_shape=jax.ShapeDtypeStruct((rows, dim), BF16),
        in_specs=[vmem] * 3 + [hbm] * 7 + [vmem] * 4,
        out_specs=vmem,
        scratch_shapes=[
            pltpu.VMEM((dim, (n_q + 2) * head), BF16),
            pltpu.VMEM((n_q * head, dim), BF16),
            pltpu.VMEM((dim, ffn), BF16),
            pltpu.VMEM((dim, ffn), BF16),
            pltpu.VMEM((ffn, dim), BF16),
            pltpu.VMEM((n_dev,) + block, BF16),
            pltpu.VMEM((n_dev,) + block, BF16),
            pltpu.VMEM((seq_len, head), F32),
            pltpu.VMEM((seq_len, head), F32),
            pltpu.VMEM((seq_len, head), jnp.int32),
            pltpu.VMEM((chips,) + block, BF16),
            pltpu.VMEM((chips,) + block, BF16),
            pltpu.VMEM((chips,) + block, BF16),
            pltpu.VMEM((chips - 1,) + block, BF16),
            pltpu.VMEM((2 * (chips - 1),) + block, BF16),
            pltpu.VMEM((chips, n_q, 2 * rows, head), BF16),
            pltpu.VMEM((seq_len, head), BF16),
            pltpu.VMEM((seq_len, head), BF16),
            pltpu.VMEM((2 * rows, n_q * head), BF16),
            pltpu.VMEM((2 * rows, ffn), BF16),
            pltpu.VMEM(block, BF16),
            pltpu.VMEM(block, BF16),
            dma((n_q + 6,)),
            dma((chips - 1, PIECES)),
            dma((chips - 1, PIECES)),
            dma((chips, PIECES)),
            dma((chips, PIECES)),
            dma((chips - 1, PIECES)),
            dma((2 * (chips - 1), PIECES)),
            dma((chips, PIECES)),
            dma((chips, PIECES)),
        ],
        compiler_params=pltpu.CompilerParams(collective_id=0, has_side_effects=True, vmem_limit_bytes=46 * 1024 * 1024),
    )(
        pltpu.with_memory_space_constraint(part.reshape((n_dev,) + block), pltpu.VMEM), freq, positions, *weights, g1.reshape(1, dim), g2.reshape(1, dim), g3.reshape(1, dim), g4.reshape(1, dim),
    )


def solution(mesh):
    n_dev = mesh.shape["tp"]
    in_specs = (P("dp", None), P("dp", None), P("tp", None), P(None, "tp", None), P(None, "tp", None), P(None, "tp", None), P("tp", None, None), P(None, "tp"), P(None, "tp"), P("tp", None), P(None), P(None), P(None), P(None))

    def device_step(tokens, positions, embed_block, *weights):
        part = lookup(tokens, embed_block)
        return decoder_layer(n_dev, part, positions, *weights)[None]

    return jax.shard_map(device_step, mesh=mesh, in_specs=in_specs, out_specs=P("dp", "tp", None), check_vma=False)
```
